256 devices in a mesh: group: 2 (over y), expert: 32 (over z, core), tensor: 4 (over x).
Axes of the slice: x: 4, y: 2, z: 16, core: 2. Of those that a mesh axis runs over, the one named last changes fastest.
The devices are a block of a 4x16x16 slice.
Arguments:
- tokens: bfloat16 [16384, 4096], P(('group', 'expert', 'tensor')), parts along dimension 0, may hold values from -6 to 6
- cotangent: bfloat16 [16384, 4096], P(('group', 'expert', 'tensor')), parts along dimension 0, may hold values from -6 to 6
- expert_ids: int32 [16384, 2], P(('group', 'expert', 'tensor')), parts along dimension 0, may hold values from 0 to 31, all different within a row
- gate_wts: float32 [16384, 2], P(('group', 'expert', 'tensor')), parts along dimension 0, may hold values from 0.2 to 1
- w_gate: bfloat16 [32, 4096, 256], P('expert', 'tensor'), may hold values from -0.09375 to 0.09375
- w_up: bfloat16 [32, 4096, 256], P('expert', 'tensor'), may hold values from -0.09375 to 0.09375
- w_down: bfloat16 [32, 256, 4096], P('expert', 'tensor'), may hold values from -0.375 to 0.375
Outputs:
- input_grad: bfloat16 [16384, 4096], P(('group', 'expert', 'tensor')), parts along dimension 0
- grad_gate: bfloat16 [64, 4096, 256], P(('group', 'expert'), 'tensor'), parts along dimension 0
- grad_up: bfloat16 [64, 4096, 256], P(('group', 'expert'), 'tensor'), parts along dimension 0
- grad_down: bfloat16 [64, 256, 4096], P(('group', 'expert'), 'tensor'), parts along dimension 0
The draws below stay inside these ranges and needn't reach their ends.
There are 2 independent parts, one for each index of `group`. The reference program is written for one: setup_inputs(seed, part) draws one part's arguments, and reference() takes and returns one part's arrays. A program takes and returns all parts, laid end to end along the dimension named above; an argument that names none is the same for every part. Nothing has to cross between parts.
Inputs may be any that keep to these rules, and one draw needn't show every extreme that they name: `expert_ids`: the two ids of a token differ.
All inputs are finite; a program needn't handle non-finite values.
Results may differ from the reference program's by a relative error of at most 0.009.
Values may be sent and summed in bfloat16 or wider, within the bound.
No kernel may reach another device: no remote copies, remote signals or barrier semaphores. Data moves between devices by JAX's collectives and lax.ppermute only.
A program may use at most 64 MiB of HBM per device.

```python
import jax
import jax.numpy as jnp
from jax import lax

D = 4096
FF = 256
TOK_DEV = 64
EXPERTS = 32
CAP = 4
TOKENS = 8192
N_EXPERT = 32
N_TENSOR = 4


def block_levels(key, shape, pieces, least, top_value):
    factor_of, own = 1.0, jax.random.fold_in(key, 6)
    for position, blocks in pieces:
        steps = jnp.exp(jax.random.uniform(jax.random.fold_in(own, position), (blocks,), jnp.float32, least / len(pieces), top_value / len(pieces)))
        factor_of = factor_of * jnp.repeat(steps, shape[position] // blocks).reshape([-1 if axis == position else 1 for axis in range(len(shape))])
    return factor_of


def different_ones(key, rows, amount, top, lift):
    ranking = jax.random.permutation(jax.random.fold_in(key, 1), amount)
    pull = ranking
    for power in range(3):
        pull = pull * pull // amount
    pull = pull * lift // amount
    chance = jax.random.randint(jax.random.fold_in(key, 2), (rows, amount), 0, 4096) + pull
    holders = jax.random.permutation(jax.random.fold_in(key, 3), rows)[jnp.arange(amount) % rows]
    chance = jnp.where(jnp.arange(rows)[:, None] == holders[None, :], 1 << 14, chance)
    priority = chance * amount + jnp.arange(amount)
    return lax.top_k(priority.astype(jnp.int32), top)[1].astype(jnp.int32)


def gaussian(stream_key, extent, spread, limit, pieces=(), kind=jnp.bfloat16):
    level = block_levels(stream_key, extent, pieces, -0.22, 0.18) if pieces else 1.0
    drawn = jax.random.normal(stream_key, extent, jnp.float32) * spread * level
    return jnp.minimum(jnp.maximum(drawn, -limit), limit).astype(kind)


def setup_inputs(seed: int = 0, part: int = 0) -> dict:
    seeds = jax.random.split(jax.random.key(seed), 8)
    part_splits = jax.random.split(jax.random.fold_in(seeds[7], part), 8)
    return {
        "tokens": gaussian(part_splits[0], (TOKENS, D), 1.0, 6.0, ((0, 128),)),
        "cotangent": gaussian(part_splits[1], (TOKENS, D), 1.0, 6.0, ((0, 128),)),
        "expert_ids": different_ones(part_splits[2], TOKENS, EXPERTS, 2, 512),
        "gate_wts": jnp.clip(0.2 + 0.8 * jax.random.uniform(part_splits[3], (TOKENS, 2), jnp.float32) ** block_levels(part_splits[3], (TOKENS, 2), ((0, 128),), -0.2, 0.2), 0.2, 1.0),
        "w_gate": gaussian(seeds[4], (EXPERTS, D, FF), D ** -0.5, 0.09375, ((0, 32), (1, 4))),
        "w_up": gaussian(seeds[5], (EXPERTS, D, FF), D ** -0.5, 0.09375, ((0, 32), (1, 4))),
        "w_down": gaussian(seeds[6], (EXPERTS, FF, D), FF ** -0.5, 0.375, ((0, 32), (1, 4))),
    }


def reference(tokens, cotangent, expert_ids, gate_wts, w_gate, w_up, w_down):
    sources = N_EXPERT * N_TENSOR
    model_width = tokens.shape[1]
    slots_all = EXPERTS * CAP
    flat_ids = expert_ids.reshape(sources, 2 * TOK_DEV)
    onehot = (flat_ids[:, :, None] == jnp.arange(EXPERTS, dtype=jnp.int32)[None, None, :]).astype(jnp.int32)
    positions = jnp.sum(onehot * (jnp.cumsum(onehot, axis=1) - 1), axis=2)
    retained = positions < CAP
    target = jnp.where(retained, flat_ids * CAP + positions, slots_all)

    def invert(row_target):
        return jnp.full((slots_all,), -1, jnp.int32).at[row_target].set(
            jnp.arange(2 * TOK_DEV, dtype=jnp.int32), mode="drop")

    anchor = jax.vmap(invert)(target)
    gate_flat = gate_wts.reshape(sources, 2 * TOK_DEV)
    block_base = (jnp.arange(sources, dtype=jnp.int32) * TOK_DEV)[:, None]
    zero_half = jnp.zeros((), jnp.bfloat16)

    def partial_sum(left, right):
        left_transposed = left.reshape(N_EXPERT, N_TENSOR, CAP, -1).transpose(1, 0, 2, 3)
        left_transposed = left_transposed.reshape(N_TENSOR, N_EXPERT * CAP, -1).astype(jnp.float32)
        right_transposed = right.reshape(N_EXPERT, N_TENSOR, CAP, -1).transpose(1, 0, 2, 3)
        right_transposed = right_transposed.reshape(N_TENSOR, N_EXPERT * CAP, -1).astype(jnp.float32)
        summands = jnp.einsum("aye,aym->aem", left_transposed, right_transposed).astype(jnp.bfloat16)
        summands = lax.optimization_barrier(summands)
        return jnp.sum(summands.astype(jnp.float32), axis=0).astype(jnp.bfloat16)

    def one_expert(expert):
        chosen = lax.dynamic_slice_in_dim(anchor, expert * CAP, CAP, 1)
        populated_rows = (chosen >= 0).reshape(-1)
        picked = jnp.maximum(chosen, 0)
        tok_index = (block_base + picked // 2).reshape(-1)
        rows_in = jnp.where(populated_rows[:, None], tokens[tok_index], zero_half)
        gate_scale = jnp.take_along_axis(gate_flat, picked, axis=1).reshape(-1)
        scaled = (gate_scale[:, None] * cotangent[tok_index].astype(jnp.float32)).astype(jnp.bfloat16)
        cot_in = jnp.where(populated_rows[:, None], scaled, zero_half)
        gate_matrix = w_gate[expert]
        up_mat = w_up[expert]
        down_mat = w_down[expert]
        pre_gate = jnp.dot(rows_in, gate_matrix, preferred_element_type=jnp.float32)
        pre_up = jnp.dot(rows_in, up_mat, preferred_element_type=jnp.float32)
        sigmoid_gate = jax.nn.sigmoid(pre_gate)
        activated = pre_gate * sigmoid_gate
        hidden = (activated * pre_up).astype(jnp.bfloat16)
        grad_hidden = jnp.dot(cot_in, down_mat.T, preferred_element_type=jnp.float32)
        grad_gate_pre = (grad_hidden * pre_up * sigmoid_gate * (1.0 + pre_gate * (1.0 - sigmoid_gate))).astype(jnp.bfloat16)
        grad_up_pre = (grad_hidden * activated).astype(jnp.bfloat16)
        input_rows = (jnp.dot(grad_gate_pre, gate_matrix.T, preferred_element_type=jnp.float32)
                      + jnp.dot(grad_up_pre, up_mat.T, preferred_element_type=jnp.float32)).astype(jnp.bfloat16)
        return (partial_sum(rows_in, grad_gate_pre), partial_sum(rows_in, grad_up_pre),
                partial_sum(hidden, cot_in), input_rows.reshape(sources, CAP, model_width))

    grad_gate, grad_up, grad_down, input_all = lax.map(one_expert, jnp.arange(EXPERTS, dtype=jnp.int32))
    slot_clip = jnp.minimum(positions, CAP - 1).astype(jnp.int32)
    source_index = jnp.broadcast_to(jnp.arange(sources, dtype=jnp.int32)[:, None], flat_ids.shape)
    gathered = input_all[flat_ids, source_index, slot_clip].astype(jnp.float32)
    gathered = jnp.where(retained[:, :, None], gathered, jnp.zeros((), jnp.float32))
    input_grad = jnp.sum(gathered.reshape(sources, TOK_DEV, 2, model_width), axis=2)
    input_grad = input_grad.reshape(TOKENS, model_width).astype(jnp.bfloat16)
    return (input_grad, grad_gate, grad_up, grad_down)
```

```python
import functools

import jax
import jax.numpy as jnp
from jax import lax
from jax.experimental import pallas as pl
from jax.experimental.pallas import tpu as pltpu
from jax.sharding import PartitionSpec as P

BF = jnp.bfloat16
F32 = jnp.float32
VMEM = pl.BlockSpec(memory_space=pltpu.VMEM)
SMEM = pl.BlockSpec(memory_space=pltpu.SMEM)
SPLIT = (3, 1)


def cost(flops, bytes_accessed):
    return pl.CostEstimate(flops=int(flops), bytes_accessed=int(bytes_accessed), transcendentals=0)


def nn(a, b):
    return lax.dot_general(a, b, (((1,), (0,)), ((), ())), preferred_element_type=F32)


def nt(a, b):
    return lax.dot_general(a, b, (((1,), (1,)), ((), ())), preferred_element_type=F32)


def tn(a, b):
    return lax.dot_general(a, b, (((0,), (0,)), ((), ())), preferred_element_type=F32)


def dispatch_kernel(split, ids_ref, gate_ref, tok_ref, cot_ref, *refs):
    outs, (pick_ref, scale_ref) = refs[: len(split)], refs[len(split) :]
    n_tok, width = tok_ref.shape
    quarter = width // 4
    experts = outs[0].shape[0]
    rows = experts * 8
    slots = sum(split)

    @pl.when(pl.program_id(0) == 0)
    def _():
        row = lax.broadcasted_iota(jnp.int32, (rows, 2 * n_tok), 0)
        lane = lax.broadcasted_iota(jnp.int32, (rows, 2 * n_tok), 1)
        expert = row // 8
        first = ids_ref[0:1, :] == expert
        second = ids_ref[1:2, :] == expert
        member = jnp.where(first | second, 1.0, 0.0).astype(F32)
        j = lax.broadcasted_iota(jnp.int32, (2 * n_tok, 2 * n_tok), 0)
        c = lax.broadcasted_iota(jnp.int32, (2 * n_tok, 2 * n_tok), 1)
        earlier = jnp.where((j < n_tok) & (j < c % n_tok), 1.0, 0.0).astype(BF)
        before = nn(member.astype(BF), earlier)
        gates = jnp.where(first, gate_ref[0:1, :], gate_ref[1:2, :])
        kind = row % 2
        same_kind = kind == lane // n_tok
        part = (row % 8) // 2
        for p in range(slots):
            chosen = jnp.where(before == float(p), member, 0.0)
            weight = jnp.sum(jnp.where(lane < n_tok, chosen * gates, 0.0), axis=1, keepdims=True)
            scale_ref[p] = jnp.where(kind[:, :1] == 1, weight, 1.0)
            kept = jnp.where(same_kind, chosen, 0.0)
            for q in range(4):
                pick_ref[p, :, q * 2 * n_tok : (q + 1) * 2 * n_tok] = jnp.where(part == q, kept, 0.0).astype(BF)

    stack = []
    for q in range(4):
        cols = slice(q * quarter, (q + 1) * quarter)
        stack += [tok_ref[:, cols], cot_ref[:, cols]]
    source = jnp.concatenate(stack, axis=0)
    p = 0
    for out, count in zip(outs, split):
        for k in range(count):
            picked = nn(pick_ref[p], source) * scale_ref[p]
            out[:, 0, :, k * quarter : (k + 1) * quarter] = picked.reshape(experts, 8, quarter).astype(BF)
            p += 1


def dispatch(ids2, gates2, tokens, cotangent, experts, parts, split):
    n_tok, d = tokens.shape
    width = d // parts
    rows = experts * 8
    slots = sum(split)
    return pl.pallas_call(
        functools.partial(dispatch_kernel, split),
        grid=(parts,),
        in_specs=[
            pl.BlockSpec((2, 2 * n_tok), lambda i: (0, 0)),
            pl.BlockSpec((2, 2 * n_tok), lambda i: (0, 0)),
            pl.BlockSpec((n_tok, width), lambda i: (0, i)),
            pl.BlockSpec((n_tok, width), lambda i: (0, i)),
        ],
        out_specs=[pl.BlockSpec((experts, 1, 8, c * width // 4), lambda i: (0, i, 0, 0)) for c in split],
        out_shape=[jax.ShapeDtypeStruct((experts, parts, 8, c * width // 4), BF) for c in split],
        scratch_shapes=[pltpu.VMEM((slots, rows, 8 * n_tok), BF), pltpu.VMEM((slots, rows, 1), F32)],
        cost_estimate=cost(2 * slots * rows * 8 * n_tok * d // 4, 4 * n_tok * d * 2 + 2 * slots * experts * d * 2),
        name="dispatch",
    )(ids2, gates2, tokens, cotangent)


def project_kernel(count, t_ref, recv_ref, wg_ref, wu_ref, *refs):
    parts = 4
    wd_refs, refs = refs[:parts], refs[parts:]
    x_ref, c_ref = refs[0], refs[1]
    z_refs, (flat, wd, z) = refs[2 : 2 + parts], refs[2 + parts :]
    t = t_ref[0]
    ff_part, width = wd_refs[0].shape
    sources = recv_ref.shape[0]
    quarter = width // 4
    group = sources // parts
    for d in range(parts):
        at = pl.multiple_of(lax.rem(t - d + parts, parts) * ff_part, ff_part)
        wd[pl.ds(at, ff_part), :] = wd_refs[d][...]
    for b in range(flat.shape[0]):
        flat[b] = recv_ref[:, :, b * 128 : (b + 1) * 128].astype(F32).reshape(flat.shape[1:])
    lanes = quarter // 128
    for p in range(count):
        for kind, dst in ((0, x_ref), (1, c_ref)):
            for q in range(4):
                for b in range(lanes):
                    v = flat[p * lanes + b, pl.ds(2 * q + kind, sources, stride=8), :].astype(BF)
                    for g in range(parts):
                        r = (g * count + p) * group
                        dst[r : r + group, q * quarter + b * 128 : q * quarter + (b + 1) * 128] = v[
                            g * group : (g + 1) * group
                        ]
    ff = wg_ref.shape[1]
    per = count * group
    x = x_ref[...]
    z[:, :, 0:ff] = nn(x, wg_ref[...]).astype(BF).reshape(parts, per, ff)
    z[:, :, ff : 2 * ff] = nn(x, wu_ref[...]).astype(BF).reshape(parts, per, ff)
    z[:, :, 2 * ff :] = nt(c_ref[...], wd[...]).astype(BF).reshape(parts, per, ff)
    for d in range(parts):
        z_refs[d][...] = z[lax.rem(t + d, parts)]


def project(t, recv, wg, wu, wd_pieces, count):
    sources = recv.shape[0]
    width, ff = wg.shape
    rows = sources * count
    parts = len(wd_pieces)
    out = [jax.ShapeDtypeStruct((rows, width), BF)] * 2 + [jax.ShapeDtypeStruct((rows // parts, 3 * ff), BF)] * parts
    return pl.pallas_call(
        functools.partial(project_kernel, count),
        in_specs=[SMEM] + [VMEM] * (3 + parts),
        out_specs=[VMEM] * len(out),
        out_shape=out,
        scratch_shapes=[
            pltpu.VMEM((count * width // 4 // 128, sources * 8, 128), F32),
            pltpu.VMEM((ff, width), BF),
            pltpu.VMEM((parts, rows // parts, 3 * ff), BF),
        ],
        cost_estimate=cost(2 * rows * width * 3 * ff, 4 * rows * width * 2 + 3 * ff * width * 2),
        name="project",
    )(t, recv, wg, wu, *wd_pieces)


def middle_kernel(a_ref, b_ref, c_ref, d_ref, h_ref):
    ff = h_ref.shape[1] // 3
    total = (a_ref[...].astype(F32) + b_ref[...].astype(F32)) + (c_ref[...].astype(F32) + d_ref[...].astype(F32))
    pre_gate, pre_up, grad_hidden = total[:, :ff], total[:, ff : 2 * ff], total[:, 2 * ff :]
    sig = jax.nn.sigmoid(pre_gate)
    activated = pre_gate * sig
    h_ref[:, :ff] = (activated * pre_up).astype(BF)
    h_ref[:, ff : 2 * ff] = (grad_hidden * pre_up * sig * (1.0 + pre_gate * (1.0 - sig))).astype(BF)
    h_ref[:, 2 * ff :] = (grad_hidden * activated).astype(BF)


def middle(z):
    return pl.pallas_call(
        middle_kernel,
        in_specs=[VMEM] * 4,
        out_specs=VMEM,
        out_shape=jax.ShapeDtypeStruct(z[0].shape, BF),
        cost_estimate=cost(40 * z[0].size, 10 * z[0].size),
        name="middle",
    )(*z)


def back_kernel(count, t_ref, wg_ref, wu_ref, *refs):
    parts = 4
    h_refs, (msg_ref, all_ref, h, flat) = refs[:parts], refs[parts:]
    t = t_ref[0]
    width, ff = wg_ref.shape
    sources = msg_ref.shape[0]
    group = sources // parts
    for d in range(parts):
        h[lax.rem(t - d + parts, parts)] = h_refs[d][...]
    joint = h[...].reshape(sources * count, 3 * ff)
    all_ref[...] = joint
    eighth = width // 8
    for half in range(2):
        cols = slice(half * width // 2, (half + 1) * width // 2)
        rows = nt(joint[:, ff : 2 * ff], wg_ref[cols, :]) + nt(joint[:, 2 * ff :], wu_ref[cols, :])
        for g in range(parts):
            for p in range(count):
                r = (g * count + p) * group
                for o in range(4):
                    flat[p, pl.ds(g * group * 8 + half * 4 + o, group, stride=8), :] = rows[
                        r : r + group, o * eighth : (o + 1) * eighth
                    ]
    for p in range(count):
        msg_ref[:, :, p * eighth : (p + 1) * eighth] = flat[p].reshape(sources, 8, eighth).astype(BF)


def back(t, wg, wu, h, count):
    width, ff = wg.shape
    parts = len(h)
    rows = h[0].shape[0] * parts
    sources = rows // count
    return pl.pallas_call(
        functools.partial(back_kernel, count),
        in_specs=[SMEM] + [VMEM] * (2 + parts),
        out_specs=[VMEM] * 2,
        out_shape=[
            jax.ShapeDtypeStruct((sources, 8, count * width // 8), BF),
            jax.ShapeDtypeStruct((rows, 3 * ff), BF),
        ],
        scratch_shapes=[
            pltpu.VMEM((parts, rows // parts, 3 * ff), BF),
            pltpu.VMEM((count, sources * 8, width // 8), F32),
        ],
        cost_estimate=cost(4 * rows * width * ff, rows * width * 2 + 2 * width * ff * 2),
        name="back",
    )(t, wg, wu, *h)


def combine_kernel(split, parts, ids_ref, *refs):
    rets, refs = refs[: len(split)], refs[len(split) :]
    out_ref, flats, rhs = refs[0], refs[1 : 1 + len(split)], refs[1 + len(split)]
    n_tok, d = out_ref.shape
    slots = sum(split)
    experts = rets[0].shape[0] // parts
    eighth = d // parts // 8
    lane = lax.broadcasted_iota(jnp.int32, (n_tok, slots * experts), 1)
    expert = lane % experts
    member = jnp.where((ids_ref[:, 0:1] == expert) | (ids_ref[:, 1:2] == expert), 1.0, 0.0).astype(F32)
    i = lax.broadcasted_iota(jnp.int32, (n_tok, n_tok), 0)
    j = lax.broadcasted_iota(jnp.int32, (n_tok, n_tok), 1)
    before = nn(jnp.where(j < i, 1.0, 0.0).astype(BF), member.astype(BF))
    pick = jnp.where(before == (lane // experts).astype(F32), member, 0.0).astype(BF)
    for ret, flat in zip(rets, flats):
        for k in range(flat.shape[0]):
            flat[k] = ret[:, :, k * eighth : (k + 1) * eighth].astype(F32).reshape(flat.shape[1:])
    for u in range(parts * 8):
        p = 0
        for flat, count in zip(flats, split):
            for k in range(count):
                v = flat[k, pl.ds(u, experts, stride=parts * 8), :]
                rhs[p * experts : (p + 1) * experts, u * eighth : (u + 1) * eighth] = v.astype(BF)
                p += 1
    out_ref[...] = nn(pick, rhs[...]).astype(BF)


def combine(ids, rets, split, parts, d):
    n_tok = ids.shape[0]
    slots = sum(split)
    experts = rets[0].shape[0] // parts
    return pl.pallas_call(
        functools.partial(combine_kernel, split, parts),
        in_specs=[VMEM] * (1 + len(split)),
        out_specs=VMEM,
        out_shape=jax.ShapeDtypeStruct((n_tok, d), BF),
        scratch_shapes=[pltpu.VMEM((c, r.shape[0] * 8, d // parts // 8), F32) for c, r in zip(split, rets)]
        + [pltpu.VMEM((slots * experts, d), BF)],
        cost_estimate=cost(2 * n_tok * slots * experts * d, 4 * n_tok * d * 2),
        name="combine",
    )(ids, *rets)


def place_kernel(t_ref, *refs):
    parts = len(refs) - 1
    out = refs[-1]
    width = refs[0].shape[1]
    for d in range(parts):
        at = pl.multiple_of(lax.rem(t_ref[0] - d + parts, parts) * width, width)
        out[:, pl.ds(at, width)] = refs[d][...]


def place(t, pieces):
    rows, width = pieces[0].shape
    return pl.pallas_call(
        place_kernel,
        in_specs=[SMEM] + [VMEM] * len(pieces),
        out_specs=VMEM,
        out_shape=jax.ShapeDtypeStruct((rows, width * len(pieces)), BF),
        cost_estimate=cost(rows * width, 4 * rows * width * 4),
        name="place",
    )(t, *pieces)


def local(tokens, cotangent, expert_ids, gate_wts, w_gate, w_up, w_down):
    n_tok, d = tokens.shape
    experts = lax.axis_size("expert")
    parts = lax.axis_size("tensor")
    slots = 2 * n_tok // experts
    split = SPLIT if sum(SPLIT) == slots else (slots,)
    t = lax.axis_index("tensor").astype(jnp.int32)
    t1 = t.reshape(1)
    wg, wu, wd = w_gate[0], w_up[0], w_down[0]
    width, ff = wg.shape
    ff_part = wd.shape[0]

    def shift(x, k):
        return lax.ppermute(x, "tensor", [(s, (s + k) % parts) for s in range(parts)])

    ids2 = jnp.tile(expert_ids.T, (1, 2))
    gates2 = jnp.tile(gate_wts.T, (1, 2))
    sends = dispatch(ids2, gates2, tokens, cotangent, experts, parts, split)
    sources = experts * parts

    wd_pieces = [lax.dynamic_slice_in_dim(wd, lax.rem(t + k, parts) * width, width, 1) for k in range(parts)]
    wd_pieces = [wd_pieces[0]] + [shift(wd_pieces[k], k) for k in range(1, parts)]

    axes = ("expert", "tensor")
    x_all, c_all, h_all, rets = [], [], [], []
    for send, count in zip(sends, split):
        recv = lax.all_to_all(send.reshape(sources, 8, -1), axes, 0, 0, tiled=True)
        x, c, *z = project(t1, recv, wg, wu, wd_pieces, count)
        h = middle([z[0]] + [shift(z[k], k) for k in range(1, parts)])
        msg, joint = back(t1, wg, wu, [h] + [shift(h, k) for k in range(1, parts)], count)
        rets.append(lax.all_to_all(msg, axes, 0, 0, tiled=True))
        x_all.append(x)
        c_all.append(c)
        h_all.append(joint)

    def total(pairs):
        return functools.reduce(lambda a, b: a + b, [tn(a, b) for a, b in pairs]).astype(BF)

    grad_gate = total([(x, h[:, ff : 2 * ff]) for x, h in zip(x_all, h_all)])
    grad_up = total([(x, h[:, 2 * ff :]) for x, h in zip(x_all, h_all)])
    grad_down = total([(h[:, :ff], c) for c, h in zip(c_all, h_all)])
    pieces = [lax.dynamic_slice_in_dim(grad_down, lax.rem(t + k, parts) * ff_part, ff_part, 0) for k in range(parts)]
    grad_down = place(t1, [pieces[0]] + [shift(pieces[k], k) for k in range(1, parts)])
    input_grad = combine(expert_ids, rets, split, parts, d)
    return input_grad, grad_gate[None], grad_up[None], grad_down[None]


def solution(mesh):
    tok = P(("group", "expert", "tensor"), None)
    wts = P("expert", "tensor", None)
    out = P(("group", "expert"), "tensor", None)
    return jax.shard_map(
        local,
        mesh=mesh,
        in_specs=(tok, tok, tok, tok, wts, wts, wts),
        out_specs=(tok, out, out, out),
        check_vma=False,
    )
```

```python
import functools

import jax
import jax.numpy as jnp
from jax import lax
from jax.experimental import pallas as pl
from jax.experimental.pallas import tpu as pltpu
from jax.sharding import PartitionSpec as P

BF = jnp.bfloat16
F32 = jnp.float32
VMEM = pl.BlockSpec(memory_space=pltpu.VMEM)
SMEM = pl.BlockSpec(memory_space=pltpu.SMEM)
SPLIT = (2, 2)
PARTS = 4
STEPS = 4


def cost(flops, bytes_accessed):
    return pl.CostEstimate(flops=int(flops), bytes_accessed=int(bytes_accessed), transcendentals=0)


def nn(a, b):
    return lax.dot_general(a, b, (((1,), (0,)), ((), ())), preferred_element_type=F32)


def nt(a, b):
    return lax.dot_general(a, b, (((1,), (1,)), ((), ())), preferred_element_type=F32)


def tn(a, b):
    return lax.dot_general(a, b, (((0,), (0,)), ((), ())), preferred_element_type=F32)


def dispatch_kernel(split, ids_ref, gate_ref, *refs):
    sources, refs = refs[:8], refs[8:]
    outs, (pick_ref, scale_ref) = refs[: len(split)], refs[len(split) :]
    n_tok, lanes = sources[0].shape
    experts = outs[0].shape[0]
    rows = experts * 8
    slots = sum(split)

    @pl.when(pl.program_id(0) == 0)
    def _():
        row = lax.broadcasted_iota(jnp.int32, (rows, n_tok), 0)
        expert = row // 8
        first = ids_ref[0:1, :] == expert
        second = ids_ref[1:2, :] == expert
        member = jnp.where(first | second, 1.0, 0.0).astype(F32)
        j = lax.broadcasted_iota(jnp.int32, (n_tok, n_tok), 0)
        i = lax.broadcasted_iota(jnp.int32, (n_tok, n_tok), 1)
        before = nn(member.astype(BF), jnp.where(j < i, 1.0, 0.0).astype(BF))
        gates = jnp.where(first, gate_ref[0:1, :], gate_ref[1:2, :])
        is_cot = row % 2 == 1
        wide = lax.broadcasted_iota(jnp.int32, (rows, 2 * n_tok), 0)
        part = (wide % 8) // 2
        for p in range(slots):
            chosen = jnp.where(before == float(p), member, 0.0)
            weight = jnp.sum(chosen * gates, axis=1, keepdims=True)
            scale_ref[p] = jnp.where(is_cot[:, :1], weight, 1.0)
            kept = jnp.concatenate([jnp.where(is_cot, 0.0, chosen), jnp.where(is_cot, chosen, 0.0)], axis=1)
            for q in range(4):
                pick_ref[p, :, q * 2 * n_tok : (q + 1) * 2 * n_tok] = jnp.where(part == q, kept, 0.0).astype(BF)

    source = jnp.concatenate([s[...] for s in sources], axis=0)
    p = 0
    for out, count in zip(outs, split):
        for k in range(count):
            picked = nn(pick_ref[p], source) * scale_ref[p]
            out[:, :, k * lanes : (k + 1) * lanes] = picked.reshape(experts, 8, lanes).astype(BF)
            p += 1


def dispatch(ids2, gates2, tokens, cotangent, experts, split):
    n_tok, d = tokens.shape
    lanes = d // 4 // STEPS
    rows = experts * 8
    slots = sum(split)
    columns = []
    for q in range(4):
        columns += [pl.BlockSpec((n_tok, lanes), lambda i, q=q: (0, q * STEPS + i))] * 2
    return pl.pallas_call(
        functools.partial(dispatch_kernel, split),
        grid=(STEPS,),
        in_specs=[pl.BlockSpec((2, n_tok), lambda i: (0, 0))] * 2 + columns,
        out_specs=[pl.BlockSpec((experts, 8, c * lanes), lambda i: (0, 0, i)) for c in split],
        out_shape=[jax.ShapeDtypeStruct((experts, 8, c * d // 4), BF) for c in split],
        scratch_shapes=[pltpu.VMEM((slots, rows, 8 * n_tok), BF), pltpu.VMEM((slots, rows, 1), F32)],
        cost_estimate=cost(2 * slots * rows * 8 * n_tok * d // 4, 4 * n_tok * d * 2 + 2 * slots * experts * d * 2),
        name="dispatch",
    )(ids2, gates2, *([tokens, cotangent] * 4))


def expert_kernel(count, t_ref, recv_ref, *refs):
    wg, wu, wds, refs = refs[:PARTS], refs[PARTS : 2 * PARTS], refs[2 * PARTS : 3 * PARTS], refs[3 * PARTS :]
    msg_ref, exchange, (flat, x, c, wd, back, ret) = refs[0], refs[1 : 1 + PARTS], refs[1 + PARTS :]
    t = t_ref[0]
    width, ff = wg[0].shape
    ff_part, d_model = wds[0].shape
    sources = recv_ref.shape[0]
    rows = count * sources
    lanes = d_model // 4 // STEPS
    blocks = lanes // 128
    part = [lax.rem(t - k + PARTS, PARTS) for k in range(PARTS)]
    for k in range(PARTS):
        wd[pl.ds(pl.multiple_of(part[k] * ff_part, ff_part), ff_part), :] = wds[k][...]
    for b in range(flat.shape[0]):
        flat[b] = recv_ref[:, :, b * 128 : (b + 1) * 128].astype(F32).reshape(flat.shape[1:])
    for step in range(STEPS):
        for p in range(count):
            for b in range(blocks):
                for q in range(4):
                    col = q * (d_model // 4) + step * lanes + b * 128
                    for kind, dst in ((0, x), (1, c)):
                        v = flat[(step * count + p) * blocks + b, pl.ds(2 * q + kind, sources, stride=8), :]
                        dst[p * sources : (p + 1) * sources, col : col + 128] = v.astype(BF)
    cols = [pl.ds(pl.multiple_of(part[k] * width, width), width) for k in range(PARTS)]
    pre_gate = functools.reduce(lambda a, b: a + b, [nn(x[:, cols[k]], wg[k][...]) for k in range(PARTS)])
    pre_up = functools.reduce(lambda a, b: a + b, [nn(x[:, cols[k]], wu[k][...]) for k in range(PARTS)])
    grad_hidden = nt(c[...], wd[...])
    sig = jax.nn.sigmoid(pre_gate)
    activated = pre_gate * sig
    hidden = (activated * pre_up).astype(BF)
    grad_gate_pre = (grad_hidden * pre_up * sig * (1.0 + pre_gate * (1.0 - sig))).astype(BF)
    grad_up_pre = (grad_hidden * activated).astype(BF)
    for k in range(PARTS):
        to = lax.rem(t + k, PARTS)
        there = pl.ds(pl.multiple_of(to * width, width), width)
        exchange[k][0:rows, :] = x[:, there]
        exchange[k][rows : 2 * rows, :] = c[:, there]
        exchange[k][2 * rows :, 0:ff] = hidden
        exchange[k][2 * rows :, ff : 2 * ff] = grad_gate_pre
        exchange[k][2 * rows :, 2 * ff : 3 * ff] = grad_up_pre
        exchange[k][2 * rows :, 3 * ff :] = jnp.zeros((rows, width - 3 * ff), BF)
    for k in range(PARTS):
        back[:, cols[k]] = nt(grad_gate_pre, wg[k][...]) + nt(grad_up_pre, wu[k][...])
    eighth = d_model // 8
    for p in range(count):
        for b in range(eighth // 128):
            for o in range(8):
                col = o * eighth + b * 128
                ret[p * (eighth // 128) + b, pl.ds(o, sources, stride=8), :] = back[
                    p * sources : (p + 1) * sources, col : col + 128
                ]
    for b in range(ret.shape[0]):
        msg_ref[:, :, b * 128 : (b + 1) * 128] = ret[b].reshape(sources, 8, 128).astype(BF)


def expert_round(t, recv, wg, wu, wd, count):
    sources = recv.shape[0]
    width, ff = wg[0].shape
    ff_part, d = wd[0].shape
    rows = sources * count
    return pl.pallas_call(
        functools.partial(expert_kernel, count),
        in_specs=[SMEM] + [VMEM] * (1 + 3 * PARTS),
        out_specs=[VMEM] * (1 + PARTS),
        out_shape=[jax.ShapeDtypeStruct((sources, 8, count * d // 8), BF)]
        + [jax.ShapeDtypeStruct((3 * rows, width), BF)] * PARTS,
        scratch_shapes=[
            pltpu.VMEM((count * d // 4 // 128, sources * 8, 128), F32),
            pltpu.VMEM((rows, d), BF),
            pltpu.VMEM((rows, d), BF),
            pltpu.VMEM((ff, d), BF),
            pltpu.VMEM((rows, d), F32),
            pltpu.VMEM((count * d // 8 // 128, sources * 8, 128), F32),
        ],
        cost_estimate=cost(2 * rows * d * 5 * ff, 3 * ff * d * 2 + 5 * rows * d * 2),
        name="expert_round",
    )(t, recv, *wg, *wu, *wd)


def grads_kernel(ff, t_ref, *refs):
    n = len(refs) - (2 + PARTS) - 3
    boxes, (gg_ref, gu_ref), downs, (x, c, h) = refs[:n], refs[n : n + 2], refs[n + 2 : n + 2 + PARTS], refs[-3:]
    at = 0
    for box in boxes:
        rows = box.shape[0] // 3
        x[at : at + rows, :] = box[0:rows, :]
        c[at : at + rows, :] = box[rows : 2 * rows, :]
        h[at : at + rows, :] = box[2 * rows :, 0 : 3 * ff]
        at += rows
    gg_ref[...] = tn(x[...], h[:, ff : 2 * ff]).astype(BF)
    gu_ref[...] = tn(x[...], h[:, 2 * ff :]).astype(BF)
    hidden = h[:, 0:ff]
    down = tn(hidden, c[...]).astype(BF)
    x[0:ff, :] = down
    part = ff // PARTS
    for k in range(PARTS):
        downs[k][...] = x[pl.ds(pl.multiple_of(lax.rem(t_ref[0] + k, PARTS) * part, part), part), :]


def grads(t, boxes, ff):
    width = boxes[0].shape[1]
    rows = sum(b.shape[0] for b in boxes) // 3
    return pl.pallas_call(
        functools.partial(grads_kernel, ff),
        in_specs=[SMEM] + [VMEM] * len(boxes),
        out_specs=[VMEM] * (2 + PARTS),
        out_shape=[jax.ShapeDtypeStruct((width, ff), BF)] * 2
        + [jax.ShapeDtypeStruct((ff // PARTS, width), BF)] * PARTS,
        scratch_shapes=[
            pltpu.VMEM((rows, width), BF),
            pltpu.VMEM((rows, width), BF),
            pltpu.VMEM((rows, 3 * ff), BF),
        ],
        cost_estimate=cost(2 * rows * width * 3 * ff, 3 * rows * width * 2 + 3 * width * ff * 2),
        name="grads",
    )(t, *boxes)


def combine_kernel(split, ids_ref, *refs):
    rets, refs = refs[: len(split)], refs[len(split) :]
    out_ref, flats, rhs = refs[0], refs[1 : 1 + len(split)], refs[1 + len(split)]
    n_tok, d = out_ref.shape
    slots = sum(split)
    experts = rets[0].shape[0]
    eighth = d // 8
    blocks = eighth // 128
    lane = lax.broadcasted_iota(jnp.int32, (n_tok, slots * experts), 1)
    expert = lane % experts
    member = jnp.where((ids_ref[:, 0:1] == expert) | (ids_ref[:, 1:2] == expert), 1.0, 0.0).astype(F32)
    i = lax.broadcasted_iota(jnp.int32, (n_tok, n_tok), 0)
    j = lax.broadcasted_iota(jnp.int32, (n_tok, n_tok), 1)
    before = nn(jnp.where(j < i, 1.0, 0.0).astype(BF), member.astype(BF))
    pick = jnp.where(before == (lane // experts).astype(F32), member, 0.0).astype(BF)
    for ret, flat in zip(rets, flats):
        for b in range(flat.shape[0]):
            flat[b] = ret[:, :, b * 128 : (b + 1) * 128].astype(F32).reshape(flat.shape[1:])
    for o in range(8):
        for b in range(blocks):
            col = o * eighth + b * 128
            p = 0
            for flat, count in zip(flats, split):
                for k in range(count):
                    v = flat[k * blocks + b, pl.ds(o, experts, stride=8), :]
                    rhs[p * experts : (p + 1) * experts, col : col + 128] = v.astype(BF)
                    p += 1
    out_ref[...] = nn(pick, rhs[...]).astype(BF)


def combine(ids, rets, split, d):
    n_tok = ids.shape[0]
    slots = sum(split)
    experts = rets[0].shape[0]
    return pl.pallas_call(
        functools.partial(combine_kernel, split),
        in_specs=[VMEM] * (1 + len(split)),
        out_specs=VMEM,
        out_shape=jax.ShapeDtypeStruct((n_tok, d), BF),
        scratch_shapes=[pltpu.VMEM((c * d // 8 // 128, r.shape[0] * 8, 128), F32) for c, r in zip(split, rets)]
        + [pltpu.VMEM((slots * experts, d), BF)],
        cost_estimate=cost(2 * n_tok * slots * experts * d, 4 * n_tok * d * 2),
        name="combine",
    )(ids, *rets)


def place_kernel(t_ref, *refs):
    out = refs[-1]
    width = refs[0].shape[1]
    for k in range(PARTS):
        at = pl.multiple_of(lax.rem(t_ref[0] - k + PARTS, PARTS) * width, width)
        out[:, pl.ds(at, width)] = refs[k][...]


def place(t, pieces):
    rows, width = pieces[0].shape
    return pl.pallas_call(
        place_kernel,
        in_specs=[SMEM] + [VMEM] * len(pieces),
        out_specs=VMEM,
        out_shape=jax.ShapeDtypeStruct((rows, width * len(pieces)), BF),
        cost_estimate=cost(rows * width, 4 * rows * width * 4),
        name="place",
    )(t, *pieces)


def local(tokens, cotangent, expert_ids, gate_wts, w_gate, w_up, w_down):
    n_tok, d = tokens.shape
    experts = lax.axis_size("expert")
    slots = 2 * n_tok // experts
    split = SPLIT if sum(SPLIT) == slots else (slots,)
    t = lax.axis_index("tensor").astype(jnp.int32).reshape(1)
    ff = w_gate.shape[2]

    def shift(x, k):
        return lax.ppermute(x, "tensor", [(s, (s + k) % PARTS) for s in range(PARTS)])

    def everyone(x):
        return [x] + [shift(x, k) for k in range(1, PARTS)]

    sends = dispatch(expert_ids.T, gate_wts.T, tokens, cotangent, experts, split)
    recvs = []
    for r, send in enumerate(sends):
        with jax.named_scope(f"inbound{r}"):
            recvs.append(lax.all_to_all(send, "expert", 0, 0, tiled=True))
    wg, wu, wd = everyone(w_gate[0]), everyone(w_up[0]), everyone(w_down[0])
    boxes, rets = [], []
    for r, (recv, count) in enumerate(zip(recvs, split)):
        with jax.named_scope(f"round{r}"):
            msg, *box = expert_round(t, recv, wg, wu, wd, count)
        with jax.named_scope(f"outbound{r}"):
            rets.append(lax.all_to_all(msg, "expert", 0, 0, tiled=True))
        with jax.named_scope(f"exchange{r}"):
            boxes += [box[0]] + [shift(box[k], k) for k in range(1, PARTS)]
    grad_gate, grad_up, *down = grads(t, boxes, ff)
    grad_down = place(t, [down[0]] + [shift(down[k], k) for k in range(1, PARTS)])
    input_grad = combine(expert_ids, rets, split, d)
    return input_grad, grad_gate[None], grad_up[None], grad_down[None]


def solution(mesh):
    tok = P(("group", "expert", "tensor"), None)
    wts = P("expert", "tensor", None)
    out = P(("group", "expert"), "tensor", None)

    return jax.shard_map(
        local,
        mesh=mesh,
        in_specs=(tok, tok, tok, tok, wts, wts, wts),
        out_specs=(tok, out, out, out),
        check_vma=False,
    )
```

```python
import functools

import jax
import jax.numpy as jnp
from jax import lax
from jax.experimental import pallas as pl
from jax.experimental.pallas import tpu as pltpu
from jax.sharding import PartitionSpec as P


BF = jnp.bfloat16
F32 = jnp.float32
VMEM = pl.BlockSpec(memory_space=pltpu.VMEM)
SMEM = pl.BlockSpec(memory_space=pltpu.SMEM)
SPLIT = (4,)
PARTS = 4
STEPS = 4


def cost(flops, bytes_accessed):
    return pl.CostEstimate(flops=int(flops), bytes_accessed=int(bytes_accessed), transcendentals=0)


def nn(a, b):
    return lax.dot_general(a, b, (((1,), (0,)), ((), ())), preferred_element_type=F32)


def nt(a, b):
    return lax.dot_general(a, b, (((1,), (1,)), ((), ())), preferred_element_type=F32)


def tn(a, b):
    return lax.dot_general(a, b, (((0,), (0,)), ((), ())), preferred_element_type=F32)


def dispatch_kernel(split, ids_ref, gate_ref, *refs):
    sources, refs = refs[:8], refs[8:]
    outs, (pick_ref, scale_ref) = refs[: len(split)], refs[len(split) :]
    n_tok, lanes = sources[0].shape
    experts = outs[0].shape[0]
    rows = experts * 8
    slots = sum(split)

    @pl.when(pl.program_id(0) == 0)
    def _():
        row = lax.broadcasted_iota(jnp.int32, (rows, n_tok), 0)
        expert = row // 8
        first = ids_ref[0:1, :] == expert
        second = ids_ref[1:2, :] == expert
        member = jnp.where(first | second, 1.0, 0.0).astype(F32)
        j = lax.broadcasted_iota(jnp.int32, (n_tok, n_tok), 0)
        i = lax.broadcasted_iota(jnp.int32, (n_tok, n_tok), 1)
        before = nn(member.astype(BF), jnp.where(j < i, 1.0, 0.0).astype(BF))
        gates = jnp.where(first, gate_ref[0:1, :], gate_ref[1:2, :])
        is_cot = row % 2 == 1
        wide = lax.broadcasted_iota(jnp.int32, (rows, 2 * n_tok), 0)
        part = (wide % 8) // 2
        for p in range(slots):
            chosen = jnp.where(before == float(p), member, 0.0)
            weight = jnp.sum(chosen * gates, axis=1, keepdims=True)
            scale_ref[p] = jnp.where(is_cot[:, :1], weight, 1.0)
            kept = jnp.concatenate([jnp.where(is_cot, 0.0, chosen), jnp.where(is_cot, chosen, 0.0)], axis=1)
            for q in range(4):
                pick_ref[p, :, q * 2 * n_tok : (q + 1) * 2 * n_tok] = jnp.where(part == q, kept, 0.0).astype(BF)

    source = jnp.concatenate([s[...] for s in sources], axis=0)
    p = 0
    for out, count in zip(outs, split):
        for k in range(count):
            picked = nn(pick_ref[p], source) * scale_ref[p]
            out[:, :, k * lanes : (k + 1) * lanes] = picked.reshape(experts, 8, lanes).astype(BF)
            p += 1


def dispatch(ids2, gates2, tokens, cotangent, experts, split):
    n_tok, d = tokens.shape
    lanes = d // 4 // STEPS
    rows = experts * 8
    slots = sum(split)
    columns = []
    for q in range(4):
        columns += [pl.BlockSpec((n_tok, lanes), lambda i, q=q: (0, q * STEPS + i))] * 2
    return pl.pallas_call(
        functools.partial(dispatch_kernel, split),
        grid=(STEPS,),
        in_specs=[pl.BlockSpec((2, n_tok), lambda i: (0, 0))] * 2 + columns,
        out_specs=[pl.BlockSpec((experts, 8, c * lanes), lambda i: (0, 0, i)) for c in split],
        out_shape=[jax.ShapeDtypeStruct((experts, 8, c * d // 4), BF) for c in split],
        scratch_shapes=[pltpu.VMEM((slots, rows, 8 * n_tok), BF), pltpu.VMEM((slots, rows, 1), F32)],
        cost_estimate=cost(2 * slots * rows * 8 * n_tok * d // 4, 4 * n_tok * d * 2 + 2 * slots * experts * d * 2),
        name="dispatch",
    )(ids2, gates2, *([tokens, cotangent] * 4))


def stack_kernel(t_ref, *refs):
    out = refs[-1]
    part = refs[0].shape[0]
    for k in range(PARTS):
        at = pl.multiple_of(lax.rem(t_ref[0] - k + PARTS, PARTS) * part, part)
        out[pl.ds(at, part), :] = refs[k][...]


def stack_down(t, pieces):
    part, d = pieces[0].shape
    return pl.pallas_call(
        stack_kernel,
        in_specs=[SMEM] + [VMEM] * PARTS,
        out_specs=VMEM,
        out_shape=jax.ShapeDtypeStruct((part * PARTS, d), BF),
        cost_estimate=cost(part * d, 4 * part * d * 4),
        name="stack_down",
    )(t, *pieces)


def expert_kernel(count, t_ref, recv_ref, *refs):
    wg, wu, wd, refs = refs[:PARTS], refs[PARTS : 2 * PARTS], refs[2 * PARTS], refs[2 * PARTS + 1 :]
    msg_ref, exchange, (flat, x, c, back, ret) = refs[0], refs[1 : 1 + PARTS], refs[1 + PARTS :]
    t = t_ref[0]
    width, ff = wg[0].shape
    d_model = wd.shape[1]
    sources = recv_ref.shape[0]
    rows = count * sources
    lanes = d_model // 4 // STEPS
    blocks = lanes // 128
    part = [lax.rem(t - k + PARTS, PARTS) for k in range(PARTS)]
    for b in range(flat.shape[0]):
        flat[b] = recv_ref[:, :, b * 128 : (b + 1) * 128].astype(F32).reshape(flat.shape[1:])
    for step in range(STEPS):
        for p in range(count):
            for b in range(blocks):
                for q in range(4):
                    col = q * (d_model // 4) + step * lanes + b * 128
                    for kind, dst in ((0, x), (1, c)):
                        v = flat[(step * count + p) * blocks + b, pl.ds(2 * q + kind, sources, stride=8), :]
                        dst[p * sources : (p + 1) * sources, col : col + 128] = v.astype(BF)
    cols = [pl.ds(pl.multiple_of(part[k] * width, width), width) for k in range(PARTS)]
    pre_gate = functools.reduce(lambda a, b: a + b, [nn(x[:, cols[k]], wg[k][...]) for k in range(PARTS)])
    pre_up = functools.reduce(lambda a, b: a + b, [nn(x[:, cols[k]], wu[k][...]) for k in range(PARTS)])
    grad_hidden = nt(c[...], wd[...])
    sig = jax.nn.sigmoid(pre_gate)
    activated = pre_gate * sig
    hidden = (activated * pre_up).astype(BF)
    grad_gate_pre = (grad_hidden * pre_up * sig * (1.0 + pre_gate * (1.0 - sig))).astype(BF)
    grad_up_pre = (grad_hidden * activated).astype(BF)
    for k in range(PARTS):
        to = lax.rem(t + k, PARTS)
        there = pl.ds(pl.multiple_of(to * width, width), width)
        exchange[k][0:rows, :] = x[:, there]
        exchange[k][rows : 2 * rows, :] = c[:, there]
        exchange[k][2 * rows :, 0:ff] = hidden
        exchange[k][2 * rows :, ff : 2 * ff] = grad_gate_pre
        exchange[k][2 * rows :, 2 * ff : 3 * ff] = grad_up_pre
        exchange[k][2 * rows :, 3 * ff :] = jnp.zeros((rows, width - 3 * ff), BF)
    for k in range(PARTS):
        back[:, cols[k]] = nt(grad_gate_pre, wg[k][...]) + nt(grad_up_pre, wu[k][...])
    eighth = d_model // 8
    for p in range(count):
        for b in range(eighth // 128):
            for o in range(8):
                col = o * eighth + b * 128
                ret[p * (eighth // 128) + b, pl.ds(o, sources, stride=8), :] = back[
                    p * sources : (p + 1) * sources, col : col + 128
                ]
    for b in range(ret.shape[0]):
        msg_ref[:, :, b * 128 : (b + 1) * 128] = ret[b].reshape(sources, 8, 128).astype(BF)


def expert_round(t, recv, wg, wu, wd, count):
    sources = recv.shape[0]
    width, ff = wg[0].shape
    d = wd.shape[1]
    rows = sources * count
    return pl.pallas_call(
        functools.partial(expert_kernel, count),
        in_specs=[SMEM] + [VMEM] * (2 + 2 * PARTS),
        out_specs=[VMEM] * (1 + PARTS),
        out_shape=[jax.ShapeDtypeStruct((sources, 8, count * d // 8), BF)]
        + [jax.ShapeDtypeStruct((3 * rows, width), BF)] * PARTS,
        scratch_shapes=[
            pltpu.VMEM((count * d // 4 // 128, sources * 8, 128), F32),
            pltpu.VMEM((rows, d), BF),
            pltpu.VMEM((rows, d), BF),
            pltpu.VMEM((rows, d), F32),
            pltpu.VMEM((count * d // 8 // 128, sources * 8, 128), F32),
        ],
        cost_estimate=cost(2 * rows * d * 5 * ff, 3 * ff * d * 2 + 5 * rows * d * 2),
        name="expert_round",
    )(t, recv, *wg, *wu, wd)


def grads_kernel(ff, t_ref, *refs):
    n = len(refs) - (2 + PARTS) - 3
    boxes, (gg_ref, gu_ref), downs, (x, c, h) = refs[:n], refs[n : n + 2], refs[n + 2 : n + 2 + PARTS], refs[-3:]
    at = 0
    for box in boxes:
        rows = box.shape[0] // 3
        x[at : at + rows, :] = box[0:rows, :]
        c[at : at + rows, :] = box[rows : 2 * rows, :]
        h[at : at + rows, :] = box[2 * rows :, 0 : 3 * ff]
        at += rows
    gg_ref[...] = tn(x[...], h[:, ff : 2 * ff]).astype(BF)
    gu_ref[...] = tn(x[...], h[:, 2 * ff :]).astype(BF)
    hidden = h[:, 0:ff]
    down = tn(hidden, c[...]).astype(BF)
    x[0:ff, :] = down
    part = ff // PARTS
    for k in range(PARTS):
        downs[k][...] = x[pl.ds(pl.multiple_of(lax.rem(t_ref[0] + k, PARTS) * part, part), part), :]


def grads(t, boxes, ff):
    width = boxes[0].shape[1]
    rows = sum(b.shape[0] for b in boxes) // 3
    return pl.pallas_call(
        functools.partial(grads_kernel, ff),
        in_specs=[SMEM] + [VMEM] * len(boxes),
        out_specs=[VMEM] * (2 + PARTS),
        out_shape=[jax.ShapeDtypeStruct((width, ff), BF)] * 2
        + [jax.ShapeDtypeStruct((ff // PARTS, width), BF)] * PARTS,
        scratch_shapes=[
            pltpu.VMEM((rows, width), BF),
            pltpu.VMEM((rows, width), BF),
            pltpu.VMEM((rows, 3 * ff), BF),
        ],
        cost_estimate=cost(2 * rows * width * 3 * ff, 3 * rows * width * 2 + 3 * width * ff * 2),
        name="grads",
    )(t, *boxes)


def combine_kernel(split, ids_ref, *refs):
    rets, refs = refs[: len(split)], refs[len(split) :]
    out_ref, flats, rhs = refs[0], refs[1 : 1 + len(split)], refs[1 + len(split)]
    n_tok, d = out_ref.shape
    slots = sum(split)
    experts = rets[0].shape[0]
    eighth = d // 8
    blocks = eighth // 128
    lane = lax.broadcasted_iota(jnp.int32, (n_tok, slots * experts), 1)
    expert = lane % experts
    member = jnp.where((ids_ref[:, 0:1] == expert) | (ids_ref[:, 1:2] == expert), 1.0, 0.0).astype(F32)
    i = lax.broadcasted_iota(jnp.int32, (n_tok, n_tok), 0)
    j = lax.broadcasted_iota(jnp.int32, (n_tok, n_tok), 1)
    before = nn(jnp.where(j < i, 1.0, 0.0).astype(BF), member.astype(BF))
    pick = jnp.where(before == (lane // experts).astype(F32), member, 0.0).astype(BF)
    for ret, flat in zip(rets, flats):
        for b in range(flat.shape[0]):
            flat[b] = ret[:, :, b * 128 : (b + 1) * 128].astype(F32).reshape(flat.shape[1:])
    for o in range(8):
        for b in range(blocks):
            col = o * eighth + b * 128
            p = 0
            for flat, count in zip(flats, split):
                for k in range(count):
                    v = flat[k * blocks + b, pl.ds(o, experts, stride=8), :]
                    rhs[p * experts : (p + 1) * experts, col : col + 128] = v.astype(BF)
                    p += 1
    out_ref[...] = nn(pick, rhs[...]).astype(BF)


def combine(ids, rets, split, d):
    n_tok = ids.shape[0]
    slots = sum(split)
    experts = rets[0].shape[0]
    return pl.pallas_call(
        functools.partial(combine_kernel, split),
        in_specs=[VMEM] * (1 + len(split)),
        out_specs=VMEM,
        out_shape=jax.ShapeDtypeStruct((n_tok, d), BF),
        scratch_shapes=[pltpu.VMEM((c * d // 8 // 128, r.shape[0] * 8, 128), F32) for c, r in zip(split, rets)]
        + [pltpu.VMEM((slots * experts, d), BF)],
        cost_estimate=cost(2 * n_tok * slots * experts * d, 4 * n_tok * d * 2),
        name="combine",
    )(ids, *rets)


def place_kernel(t_ref, *refs):
    out = refs[-1]
    width = refs[0].shape[1]
    for k in range(PARTS):
        at = pl.multiple_of(lax.rem(t_ref[0] - k + PARTS, PARTS) * width, width)
        out[:, pl.ds(at, width)] = refs[k][...]


def place(t, pieces):
    rows, width = pieces[0].shape
    return pl.pallas_call(
        place_kernel,
        in_specs=[SMEM] + [VMEM] * len(pieces),
        out_specs=VMEM,
        out_shape=jax.ShapeDtypeStruct((rows, width * len(pieces)), BF),
        cost_estimate=cost(rows * width, 4 * rows * width * 4),
        name="place",
    )(t, *pieces)


def local(tokens, cotangent, expert_ids, gate_wts, w_gate, w_up, w_down):
    n_tok, d = tokens.shape
    experts = lax.axis_size("expert")
    slots = 2 * n_tok // experts
    split = SPLIT if sum(SPLIT) == slots else (slots,)
    t = lax.axis_index("tensor").astype(jnp.int32).reshape(1)
    ff = w_gate.shape[2]

    def shift(x, k):
        return lax.ppermute(x, "tensor", [(s, (s + k) % PARTS) for s in range(PARTS)])

    def everyone(x):
        return [x] + [shift(x, k) for k in range(1, PARTS)]

    sends = dispatch(expert_ids.T, gate_wts.T, tokens, cotangent, experts, split)
    recvs = []
    for send in sends:
        recvs.append(lax.all_to_all(send, "expert", 0, 0, tiled=True))
    wg, wu, wd = everyone(w_gate[0]), everyone(w_up[0]), everyone(w_down[0])
    wd = stack_down(t, wd)
    boxes, rets = [], []
    for recv, count in zip(recvs, split):
        msg, *box = expert_round(t, recv, wg, wu, wd, count)
        rets.append(lax.all_to_all(msg, "expert", 0, 0, tiled=True))
        boxes += [box[0]] + [shift(box[k], k) for k in range(1, PARTS)]
    grad_gate, grad_up, *down = grads(t, boxes, ff)
    grad_down = place(t, [down[0]] + [shift(down[k], k) for k in range(1, PARTS)])
    input_grad = combine(expert_ids, rets, split, d)
    return input_grad, grad_gate[None], grad_up[None], grad_down[None]


def solution(mesh):
    tok = P(("group", "expert", "tensor"), None)
    wts = P("expert", "tensor", None)
    out = P(("group", "expert"), "tensor", None)

    return jax.shard_map(
        local,
        mesh=mesh,
        in_specs=(tok, tok, tok, tok, wts, wts, wts),
        out_specs=(tok, out, out, out),
        check_vma=False,
    )
```

```python
import functools

import jax
import jax.numpy as jnp
from jax import lax
from jax.experimental import pallas as pl
from jax.experimental.pallas import tpu as pltpu
from jax.sharding import PartitionSpec as P


BF = jnp.bfloat16
F32 = jnp.float32
VMEM = pl.BlockSpec(memory_space=pltpu.VMEM)
SMEM = pl.BlockSpec(memory_space=pltpu.SMEM)
PARTS = 4
STEPS = 4
NEAR = 5


def cost(flops, bytes_accessed):
    return pl.CostEstimate(flops=int(flops), bytes_accessed=int(bytes_accessed), transcendentals=0)


def nn(a, b):
    return lax.dot_general(a, b, (((1,), (0,)), ((), ())), preferred_element_type=F32)


def nt(a, b):
    return lax.dot_general(a, b, (((1,), (1,)), ((), ())), preferred_element_type=F32)


def tn(a, b):
    return lax.dot_general(a, b, (((0,), (0,)), ((), ())), preferred_element_type=F32)


def struct(*shape):
    return jax.ShapeDtypeStruct(shape, BF)


def padded(n):
    return -(-n // 16) * 16


def dispatch_kernel(slots, at_ref, ids_o, ids_p, gate_o, gate_p, *refs):
    sources, refs = refs[:4], refs[4:]
    outs, (pick_ref, scale_ref) = refs[:-2], refs[-2:]
    n_tok = sources[0].shape[0]
    per = 4 * slots
    far = len(outs)
    rows = per * far

    @pl.when(pl.program_id(0) == 0)
    def _():
        z, core = at_ref[1], at_ref[2]
        row = lax.broadcasted_iota(jnp.int32, (rows, 2 * n_tok), 0)
        lane = lax.broadcasted_iota(jnp.int32, (rows, 2 * n_tok), 1)
        expert = 2 * ((z + row // per) % far) + core
        ids = jnp.concatenate([ids_o[...], ids_p[...]], axis=1)
        gate = jnp.concatenate([gate_o[...], gate_p[...]], axis=1)
        from_core = jnp.where(lane < n_tok, core, 1 - core)
        same = (row % (2 * slots)) // slots == from_core
        first = ids[0:1, :] == expert
        second = ids[1:2, :] == expert
        member = jnp.where((first | second) & same, 1.0, 0.0).astype(F32)
        j = lax.broadcasted_iota(jnp.int32, (2 * n_tok, 2 * n_tok), 0)
        i = lax.broadcasted_iota(jnp.int32, (2 * n_tok, 2 * n_tok), 1)
        earlier = jnp.where((j < i) & (j // n_tok == i // n_tok), 1.0, 0.0).astype(BF)
        before = nn(member.astype(BF), earlier)
        chosen = jnp.where(before == (row % slots).astype(F32), member, 0.0)
        weight = jnp.sum(chosen * jnp.where(first, gate[0:1, :], gate[1:2, :]), axis=1, keepdims=True)
        is_cot = (row % per) // (2 * slots) == 1
        scale_ref[...] = jnp.where(is_cot[:, :1], weight, 1.0)
        pick_ref[:, : 2 * n_tok] = jnp.where(is_cot, 0.0, chosen).astype(BF)
        pick_ref[:, 2 * n_tok :] = jnp.where(is_cot, chosen, 0.0).astype(BF)

    source = jnp.concatenate([s[...] for s in sources], axis=0)
    picked = (nn(pick_ref[...], source) * scale_ref[...]).astype(BF)
    for k, out in enumerate(outs):
        out[...] = picked[k * per : (k + 1) * per]


def dispatch(at, ids, gates, tokens, cotangents, far, slots):
    n_tok, d = tokens[0].shape
    lanes = d // STEPS
    rows = 4 * slots * far
    small = pl.BlockSpec((2, n_tok), lambda i: (0, 0))
    return pl.pallas_call(
        functools.partial(dispatch_kernel, slots),
        grid=(STEPS,),
        in_specs=[SMEM] + [small] * 4 + [pl.BlockSpec((n_tok, lanes), lambda i: (0, i))] * 4,
        out_specs=[pl.BlockSpec((4 * slots, lanes), lambda i: (0, i))] * far,
        out_shape=[struct(4 * slots, d)] * far,
        scratch_shapes=[pltpu.VMEM((rows, 4 * n_tok), BF), pltpu.VMEM((rows, 1), F32)],
        cost_estimate=cost(2 * rows * 4 * n_tok * d, 4 * n_tok * d * 2 + rows * d * 2),
        name="dispatch",
    )(at, *ids, *gates, *tokens, *cotangents)


def pack_kernel(wg_ref, wu_ref, wd_ref, out):
    width, ff = wg_ref.shape
    part = wd_ref.shape[0]
    out[0:width, 0:ff] = wg_ref[...]
    out[0:width, ff:] = wu_ref[...]
    for b in range(wd_ref.shape[1] // (2 * ff)):
        out[width + b * part : width + (b + 1) * part, :] = wd_ref[:, b * 2 * ff : (b + 1) * 2 * ff]


def pack(wg, wu, wd):
    width, ff = wg.shape
    rows = width + wd.size // (2 * ff)
    return pl.pallas_call(
        pack_kernel,
        in_specs=[VMEM] * 3,
        out_specs=VMEM,
        out_shape=struct(rows, 2 * ff),
        cost_estimate=cost(rows * ff, 8 * rows * ff),
        name="pack",
    )(wg, wu, wd)


def stack_kernel(width, at_ref, *refs):
    out = refs[-1]
    ff, d = out.shape
    part, lanes = ff // PARTS, 2 * ff
    for k in range(PARTS):
        at = pl.multiple_of(lax.rem(at_ref[0] - k + PARTS, PARTS) * part, part)
        for b in range(d // lanes):
            out[pl.ds(at, part), b * lanes : (b + 1) * lanes] = refs[k][width + b * part : width + (b + 1) * part, :]


def stack_down(at, packs, width, ff, d):
    return pl.pallas_call(
        functools.partial(stack_kernel, width),
        in_specs=[SMEM] + [VMEM] * PARTS,
        out_specs=VMEM,
        out_shape=struct(ff, d),
        cost_estimate=cost(ff * d, 4 * ff * d),
        name="stack_down",
    )(at, *packs)


def expert_kernel(width, at_ref, wd, *refs):
    packs, refs = refs[:PARTS], refs[PARTS:]
    n = (len(refs) - 4) // 2
    recvs, backs, (h_ref, x, c, back) = refs[:n], refs[n : 2 * n], refs[2 * n :]
    t = at_ref[0]
    ff = wd.shape[0]
    half = recvs[0].shape[0] // 2
    for i in range(n):
        v = recvs[i][...].astype(F32)
        x[i * half : (i + 1) * half, :] = v[:half]
        c[i * half : (i + 1) * half, :] = v[half:]
    rows, d = x.shape
    if n * half < rows:
        x[n * half :, :] = jnp.zeros((rows - n * half, d), F32)
        c[n * half :, :] = jnp.zeros((rows - n * half, d), F32)
    cols = [pl.ds(pl.multiple_of(lax.rem(t - k + PARTS, PARTS) * width, width), width) for k in range(PARTS)]
    pre = functools.reduce(
        lambda a, b: a + b, [nn(x[:, cols[k]].astype(BF), packs[k][0:width, :]) for k in range(PARTS)]
    )
    grad_hidden = nt(c[...].astype(BF), wd[...])
    pre_gate, pre_up = pre[:, :ff], pre[:, ff:]
    sig = jax.nn.sigmoid(pre_gate)
    activated = pre_gate * sig
    h_ref[:, 0:ff] = (activated * pre_up).astype(BF)
    h_ref[:, ff : 2 * ff] = (grad_hidden * pre_up * sig * (1.0 + pre_gate * (1.0 - sig))).astype(BF)
    h_ref[:, 2 * ff :] = (grad_hidden * activated).astype(BF)
    both = h_ref[:, ff:]
    for k in range(PARTS):
        back[:, cols[k]] = nt(both, packs[k][0:width, :])
    for i in range(n):
        backs[i][...] = back[i * half : (i + 1) * half, :].astype(BF)


def expert_round(at, wd, packs, recvs, width):
    ff, d = wd.shape
    half = recvs[0].shape[0] // 2
    n = len(recvs)
    rows = padded(n * half)
    return pl.pallas_call(
        functools.partial(expert_kernel, width),
        in_specs=[SMEM] + [VMEM] * (1 + PARTS + n),
        out_specs=[VMEM] * (n + 1),
        out_shape=[struct(half, d)] * n + [struct(rows, 3 * ff)],
        scratch_shapes=[pltpu.VMEM((rows, d), F32)] * 3,
        cost_estimate=cost(2 * rows * d * 5 * ff, 3 * ff * d * 2 + 3 * rows * d * 2),
        name="expert_round",
    )(at, wd, *packs, *recvs)


def spread_kernel(at_ref, h_ref, *refs):
    n = len(refs) - PARTS - 2
    recvs, boxes, (x, c) = refs[:n], refs[n : n + PARTS], refs[n + PARTS :]
    half = recvs[0].shape[0] // 2
    rows, d = x.shape
    width = d // PARTS
    for i in range(n):
        v = recvs[i][...].astype(F32)
        x[i * half : (i + 1) * half, :] = v[:half]
        c[i * half : (i + 1) * half, :] = v[half:]
    if n * half < rows:
        x[n * half :, :] = jnp.zeros((rows - n * half, d), F32)
        c[n * half :, :] = jnp.zeros((rows - n * half, d), F32)
    wide = h_ref.shape[1]
    for k in range(PARTS):
        there = pl.ds(pl.multiple_of(lax.rem(at_ref[0] + k, PARTS) * width, width), width)
        boxes[k][0:rows, :] = x[:, there].astype(BF)
        boxes[k][rows : 2 * rows, :] = c[:, there].astype(BF)
        boxes[k][2 * rows :, 0:wide] = h_ref[...]
        boxes[k][2 * rows :, wide:] = jnp.zeros((rows, width - wide), BF)


def spread(at, h, recvs):
    d = recvs[0].shape[1]
    rows = h.shape[0]
    return pl.pallas_call(
        spread_kernel,
        in_specs=[SMEM] + [VMEM] * (1 + len(recvs)),
        out_specs=[VMEM] * PARTS,
        out_shape=[struct(3 * rows, d // PARTS)] * PARTS,
        scratch_shapes=[pltpu.VMEM((rows, d), F32)] * 2,
        cost_estimate=cost(rows * d, 8 * rows * d),
        name="spread",
    )(at, h, *recvs)


def grads_kernel(ff, at_ref, *refs):
    n = len(refs) - (2 + PARTS) - 3
    boxes, (gg_ref, gu_ref), downs, (x, c, h) = refs[:n], refs[n : n + 2], refs[n + 2 : n + 2 + PARTS], refs[-3:]
    at = 0
    for box in boxes:
        rows = box.shape[0] // 3
        x[at : at + rows, :] = box[0:rows, :]
        c[at : at + rows, :] = box[rows : 2 * rows, :]
        h[at : at + rows, :] = box[2 * rows :, 0 : 3 * ff]
        at += rows
    gg_ref[...] = tn(x[...], h[:, ff : 2 * ff]).astype(BF)
    gu_ref[...] = tn(x[...], h[:, 2 * ff :]).astype(BF)
    x[0:ff, :] = tn(h[:, 0:ff], c[...]).astype(BF)
    part = ff // PARTS
    for k in range(PARTS):
        downs[k][...] = x[pl.ds(pl.multiple_of(lax.rem(at_ref[0] + k, PARTS) * part, part), part), :]


def grads(at, boxes, ff):
    width = boxes[0].shape[1]
    rows = sum(b.shape[0] for b in boxes) // 3
    return pl.pallas_call(
        functools.partial(grads_kernel, ff),
        in_specs=[SMEM] + [VMEM] * len(boxes),
        out_specs=[VMEM] * (2 + PARTS),
        out_shape=[struct(width, ff)] * 2 + [struct(ff // PARTS, width)] * PARTS,
        scratch_shapes=[pltpu.VMEM((rows, width), BF)] * 2 + [pltpu.VMEM((rows, 3 * ff), BF)],
        cost_estimate=cost(2 * rows * width * 3 * ff, 3 * rows * width * 2 + 3 * width * ff * 2),
        name="grads",
    )(at, *boxes)


def place_kernel(at_ref, *refs):
    out = refs[-1]
    width = refs[0].shape[1]
    for k in range(PARTS):
        at = pl.multiple_of(lax.rem(at_ref[0] - k + PARTS, PARTS) * width, width)
        out[:, pl.ds(at, width)] = refs[k][...]


def place(at, pieces):
    rows, width = pieces[0].shape
    return pl.pallas_call(
        place_kernel,
        in_specs=[SMEM] + [VMEM] * len(pieces),
        out_specs=VMEM,
        out_shape=struct(rows, width * len(pieces)),
        cost_estimate=cost(rows * width, 4 * rows * width * 4),
        name="place",
    )(at, *pieces)


def combine_kernel(slots, at_ref, ids_o, ids_p, *refs):
    rets, (own_ref, other_ref, rhs) = refs[:-3], refs[-3:]
    n_tok = own_ref.shape[0]
    far = len(rets)
    per = 2 * slots
    z, core = at_ref[1], at_ref[2]
    shape = (2 * n_tok, per * far)
    row = lax.broadcasted_iota(jnp.int32, shape, 0)
    lane = lax.broadcasted_iota(jnp.int32, shape, 1)
    expert = 2 * ((z + lane // per) % far) + core
    ids = jnp.concatenate([ids_o[...], ids_p[...]], axis=0)
    same = (lane % per) // slots == jnp.where(row < n_tok, core, 1 - core)
    member = jnp.where(((ids[:, 0:1] == expert) | (ids[:, 1:2] == expert)) & same, 1.0, 0.0).astype(F32)
    i = lax.broadcasted_iota(jnp.int32, (2 * n_tok, 2 * n_tok), 0)
    j = lax.broadcasted_iota(jnp.int32, (2 * n_tok, 2 * n_tok), 1)
    earlier = jnp.where((j < i) & (j // n_tok == i // n_tok), 1.0, 0.0).astype(BF)
    before = nn(earlier, member.astype(BF))
    pick = jnp.where(before == (lane % slots).astype(F32), member, 0.0).astype(BF)
    for k in range(far):
        rhs[k * per : (k + 1) * per, :] = rets[k][...].astype(F32)
    total = nn(pick, rhs[...].astype(BF)).astype(BF)
    own_ref[...] = total[:n_tok]
    other_ref[...] = total[n_tok:]


def combine(at, ids, rets, slots):
    n_tok = ids[0].shape[0]
    d = rets[0].shape[1]
    rows = 2 * slots * len(rets)
    return pl.pallas_call(
        functools.partial(combine_kernel, slots),
        in_specs=[SMEM] + [VMEM] * (2 + len(rets)),
        out_specs=[VMEM] * 2,
        out_shape=[struct(n_tok, d)] * 2,
        scratch_shapes=[pltpu.VMEM((rows, d), F32)],
        cost_estimate=cost(4 * n_tok * rows * d, 4 * n_tok * d * 2),
        name="combine",
    )(at, *ids, *rets)


def inward(far):
    return [d for k in range(1, far // 2) for d in (k, far - k)] + [far // 2]


def near(far):
    return [d for d in inward(far) if min(d, far - d) <= NEAR]


def beyond(far):
    return [d for d in inward(far)[::-1] if min(d, far - d) > NEAR]


def local(tokens, cotangent, expert_ids, gate_wts, w_gate, w_up, w_down):
    n_tok, d = tokens.shape
    experts = lax.axis_size("expert")
    far = experts // 2
    slots = 2 * n_tok // experts
    width, ff = w_gate.shape[1:]
    e = lax.axis_index("expert").astype(jnp.int32)
    at = jnp.stack([lax.axis_index("tensor").astype(jnp.int32), e // 2, e % 2])

    def shift(x, k):
        return lax.ppermute(x, "tensor", [(s, (s + k) % PARTS) for s in range(PARTS)])

    def zshift(x, k):
        return lax.ppermute(x, "expert", [(s, (s + 2 * k) % experts) for s in range(experts)])

    def swap(x):
        return lax.ppermute(x, "expert", [(s, s ^ 1) for s in range(experts)])

    tok_p, cot_p, ids_p, gate_p = swap(tokens), swap(cotangent), swap(expert_ids), swap(gate_wts)
    packed = pack(w_gate[0], w_up[0], w_down[0])
    sends = dispatch(
        at, (expert_ids.T, ids_p.T), (gate_wts.T, gate_p.T), (tokens, tok_p), (cotangent, cot_p), far, slots
    )
    recvs = {0: sends[0]}
    packs = [packed]
    for k in inward(far):
        recvs[k] = zshift(sends[k], k)
    for k in range(1, PARTS):
        packs.append(shift(packed, k))
    wd = stack_down(at, packs, width, ff, d)
    rets, boxes = {}, []
    for group in ([0] + near(far), beyond(far)):
        mine = [recvs[k] for k in group]
        *backs, h = expert_round(at, wd, packs, mine, width)
        for k, b in zip(group, backs):
            rets[k] = zshift(b, far - k) if k else b
        box = list(spread(at, h, mine))
        for k in range(1, PARTS):
            box[k] = shift(box[k], k)
        boxes += box
    grad_gate, grad_up, *down = grads(at, boxes, ff)
    grad_down = place(at, [down[0]] + [shift(down[k], k) for k in range(1, PARTS)])
    own, other = combine(at, (expert_ids, ids_p), [rets[k] for k in range(far)], slots)
    other = swap(other)
    input_grad = (own.astype(F32) + other.astype(F32)).astype(BF)
    return input_grad, grad_gate[None], grad_up[None], grad_down[None]


def solution(mesh):
    tok = P(("group", "expert", "tensor"), None)
    wts = P("expert", "tensor", None)
    out = P(("group", "expert"), "tensor", None)

    return jax.shard_map(
        local,
        mesh=mesh,
        in_specs=(tok, tok, tok, tok, wts, wts, wts),
        out_specs=(tok, out, out, out),
        check_vma=False,
    )
```

```python
import functools

import jax
import jax.numpy as jnp
from jax import lax
from jax.experimental import pallas as pl
from jax.experimental.pallas import tpu as pltpu
from jax.sharding import PartitionSpec as P


BF = jnp.bfloat16
F32 = jnp.float32
VMEM = pl.BlockSpec(memory_space=pltpu.VMEM)
SMEM = pl.BlockSpec(memory_space=pltpu.SMEM)
PARTS = 4
STEPS = 4


def cost(flops, bytes_accessed):
    return pl.CostEstimate(flops=int(flops), bytes_accessed=int(bytes_accessed), transcendentals=0)


def struct(*shape):
    return jax.ShapeDtypeStruct(shape, BF)


def nn(a, b):
    return lax.dot_general(a, b, (((1,), (0,)), ((), ())), preferred_element_type=F32)


def nt(a, b):
    return lax.dot_general(a, b, (((1,), (1,)), ((), ())), preferred_element_type=F32)


def tn(a, b):
    return lax.dot_general(a, b, (((0,), (0,)), ((), ())), preferred_element_type=F32)


def dispatch_kernel(split, ids_ref, gate_ref, *refs):
    sources, refs = refs[:8], refs[8:]
    outs, (pick_ref, scale_ref) = refs[: len(split)], refs[len(split) :]
    n_tok, lanes = sources[0].shape
    experts = outs[0].shape[0]
    rows = experts * 8
    slots = sum(split)

    @pl.when(pl.program_id(0) == 0)
    def _():
        row = lax.broadcasted_iota(jnp.int32, (rows, n_tok), 0)
        expert = row // 8
        first = ids_ref[0:1, :] == expert
        second = ids_ref[1:2, :] == expert
        member = jnp.where(first | second, 1.0, 0.0).astype(F32)
        j = lax.broadcasted_iota(jnp.int32, (n_tok, n_tok), 0)
        i = lax.broadcasted_iota(jnp.int32, (n_tok, n_tok), 1)
        before = nn(member.astype(BF), jnp.where(j < i, 1.0, 0.0).astype(BF))
        gates = jnp.where(first, gate_ref[0:1, :], gate_ref[1:2, :])
        is_cot = row % 2 == 1
        wide = lax.broadcasted_iota(jnp.int32, (rows, 2 * n_tok), 0)
        part = (wide % 8) // 2
        for p in range(slots):
            chosen = jnp.where(before == float(p), member, 0.0)
            weight = jnp.sum(chosen * gates, axis=1, keepdims=True)
            scale_ref[p] = jnp.where(is_cot[:, :1], weight, 1.0)
            kept = jnp.concatenate([jnp.where(is_cot, 0.0, chosen), jnp.where(is_cot, chosen, 0.0)], axis=1)
            for q in range(4):
                pick_ref[p, :, q * 2 * n_tok : (q + 1) * 2 * n_tok] = jnp.where(part == q, kept, 0.0).astype(BF)

    source = jnp.concatenate([s[...] for s in sources], axis=0)
    p = 0
    for out, count in zip(outs, split):
        for k in range(count):
            picked = nn(pick_ref[p], source) * scale_ref[p]
            out[:, :, k * lanes : (k + 1) * lanes] = picked.reshape(experts, 8, lanes).astype(BF)
            p += 1


def dispatch(ids2, gates2, tokens, cotangent, experts, split):
    n_tok, d = tokens.shape
    lanes = d // 4 // STEPS
    rows = experts * 8
    slots = sum(split)
    columns = []
    for q in range(4):
        columns += [pl.BlockSpec((n_tok, lanes), lambda i, q=q: (0, q * STEPS + i))] * 2
    return pl.pallas_call(
        functools.partial(dispatch_kernel, split),
        grid=(STEPS,),
        in_specs=[pl.BlockSpec((2, n_tok), lambda i: (0, 0))] * 2 + columns,
        out_specs=[pl.BlockSpec((experts, 8, c * lanes), lambda i: (0, 0, i)) for c in split],
        out_shape=[jax.ShapeDtypeStruct((experts, 8, c * d // 4), BF) for c in split],
        scratch_shapes=[pltpu.VMEM((slots, rows, 8 * n_tok), BF), pltpu.VMEM((slots, rows, 1), F32)],
        cost_estimate=cost(2 * slots * rows * 8 * n_tok * d // 4, 4 * n_tok * d * 2 + 2 * slots * experts * d * 2),
        name="dispatch",
    )(ids2, gates2, *([tokens, cotangent] * 4))


def stack_kernel(t_ref, *refs):
    out = refs[-1]
    part = refs[0].shape[0]
    for k in range(PARTS):
        at = pl.multiple_of(lax.rem(t_ref[0] - k + PARTS, PARTS) * part, part)
        out[pl.ds(at, part), :] = refs[k][...]


def stack_down(t, pieces):
    part, d = pieces[0].shape
    return pl.pallas_call(
        stack_kernel,
        in_specs=[SMEM] + [VMEM] * PARTS,
        out_specs=VMEM,
        out_shape=jax.ShapeDtypeStruct((part * PARTS, d), BF),
        cost_estimate=cost(part * d, 4 * part * d * 4),
        compiler_params=pltpu.CompilerParams(vmem_limit_bytes=10 << 20),
        name="stack_down",
    )(t, *pieces)


def unpack(recv_ref, flat, kinds):
    sources = recv_ref.shape[0]
    d = kinds[0][1].shape[1]
    count = kinds[0][1].shape[0] // sources
    lanes = d // 4 // STEPS
    blocks = lanes // 128
    for b in range(flat.shape[0]):
        flat[b] = recv_ref[:, :, b * 128 : (b + 1) * 128].astype(F32).reshape(flat.shape[1:])
    for step in range(STEPS):
        for p in range(count):
            for b in range(blocks):
                for q in range(4):
                    col = q * (d // 4) + step * lanes + b * 128
                    for kind, dst in kinds:
                        v = flat[(step * count + p) * blocks + b, pl.ds(2 * q + kind, sources, stride=8), :]
                        dst[p * sources : (p + 1) * sources, col : col + 128] = v.astype(BF)


def flat_scratch(recv):
    return pltpu.VMEM((recv.shape[2] // 128, recv.shape[0] * 8, 128), F32)


def expert_kernel(count, t_ref, recv_ref, *refs):
    wg, wu, wd, (msg_ref, h_ref, flat, x, c, back, ret) = (
        refs[:PARTS],
        refs[PARTS : 2 * PARTS],
        refs[2 * PARTS],
        refs[2 * PARTS + 1 :],
    )
    t = t_ref[0]
    width, ff = wg[0].shape
    d = wd.shape[1]
    sources = recv_ref.shape[0]
    unpack(recv_ref, flat, [(0, x), (1, c)])
    cols = [pl.ds(pl.multiple_of(lax.rem(t - k + PARTS, PARTS) * width, width), width) for k in range(PARTS)]
    pre_gate = functools.reduce(lambda a, b: a + b, [nn(x[:, cols[k]], wg[k][...]) for k in range(PARTS)])
    pre_up = functools.reduce(lambda a, b: a + b, [nn(x[:, cols[k]], wu[k][...]) for k in range(PARTS)])
    grad_hidden = nt(c[...], wd[...])
    sig = jax.nn.sigmoid(pre_gate)
    activated = pre_gate * sig
    grad_gate_pre = (grad_hidden * pre_up * sig * (1.0 + pre_gate * (1.0 - sig))).astype(BF)
    grad_up_pre = (grad_hidden * activated).astype(BF)
    h_ref[:, 0:ff] = (activated * pre_up).astype(BF)
    h_ref[:, ff : 2 * ff] = grad_gate_pre
    h_ref[:, 2 * ff :] = grad_up_pre
    for k in range(PARTS):
        back[:, cols[k]] = nt(grad_gate_pre, wg[k][...]) + nt(grad_up_pre, wu[k][...])
    eighth = d // 8
    for p in range(count):
        for b in range(eighth // 128):
            for o in range(8):
                col = o * eighth + b * 128
                ret[p * (eighth // 128) + b, pl.ds(o, sources, stride=8), :] = back[
                    p * sources : (p + 1) * sources, col : col + 128
                ]
    for b in range(ret.shape[0]):
        msg_ref[:, :, b * 128 : (b + 1) * 128] = ret[b].reshape(sources, 8, 128).astype(BF)


def expert_round(t, recv, wg, wu, wd, count):
    sources = recv.shape[0]
    ff, d = wd.shape
    rows = sources * count
    return pl.pallas_call(
        functools.partial(expert_kernel, count),
        in_specs=[SMEM] + [VMEM] * (2 + 2 * PARTS),
        out_specs=[VMEM] * 2,
        out_shape=[struct(sources, 8, count * d // 8), struct(rows, 3 * ff)],
        scratch_shapes=[
            flat_scratch(recv),
            pltpu.VMEM((rows, d), BF),
            pltpu.VMEM((rows, d), BF),
            pltpu.VMEM((rows, d), F32),
            pltpu.VMEM((count * d // 8 // 128, sources * 8, 128), F32),
        ],
        cost_estimate=cost(2 * rows * d * 5 * ff, 3 * ff * d * 2 + 3 * rows * d * 2),
        compiler_params=pltpu.CompilerParams(vmem_limit_bytes=28 << 20),
        name="expert_round",
    )(t, recv, *wg, *wu, wd)


def spread_kernel(kind, first, wide, t_ref, recv_ref, h_ref, *refs):
    boxes, (flat, x) = refs[:PARTS], refs[PARTS:]
    unpack(recv_ref, flat, [(kind, x)])
    rows, d = x.shape
    width = d // PARTS
    folds = width // wide
    part = rows // folds
    for k in range(PARTS):
        there = pl.ds(pl.multiple_of(lax.rem(t_ref[0] + k, PARTS) * width, width), width)
        boxes[k][0:rows, :] = x[:, there]
        for f in range(folds):
            boxes[k][rows:, f * wide : (f + 1) * wide] = h_ref[f * part : (f + 1) * part, first : first + wide]


def spread(t, recv, h, kind, first, wide):
    rows = h.shape[0]
    d = recv.shape[2] * 8 * recv.shape[0] // (2 * rows)
    width = d // PARTS
    return list(
        pl.pallas_call(
            functools.partial(spread_kernel, kind, first, wide),
            in_specs=[SMEM] + [VMEM] * 2,
            out_specs=[VMEM] * PARTS,
            out_shape=[struct(rows + rows * wide // width, width)] * PARTS,
            scratch_shapes=[flat_scratch(recv), pltpu.VMEM((rows, d), BF)],
            cost_estimate=cost(rows * d, 6 * rows * d),
            compiler_params=pltpu.CompilerParams(vmem_limit_bytes=20 << 20),
        )(t, recv, h)
    )


def join(boxes, x, h):
    rows = x.shape[0] // len(boxes)
    wide = h.shape[1]
    folds = x.shape[1] // wide
    part = rows // folds
    for i, box in enumerate(boxes):
        x[i * rows : (i + 1) * rows, :] = box[0:rows, :]
        for f in range(folds):
            h[i * rows + f * part : i * rows + (f + 1) * part, :] = box[rows:, f * wide : (f + 1) * wide]


def grads_down_kernel(t_ref, *refs):
    boxes, downs, (c, h) = refs[:PARTS], refs[PARTS : 2 * PARTS], refs[2 * PARTS :]
    join(boxes, c, h)
    ff = h.shape[1]
    c[0:ff, :] = tn(h[...], c[...]).astype(BF)
    part = ff // PARTS
    for k in range(PARTS):
        downs[k][...] = c[pl.ds(pl.multiple_of(lax.rem(t_ref[0] + k, PARTS) * part, part), part), :]


def grads_up_kernel(*refs):
    boxes, (gg_ref, gu_ref, x, h) = refs[:PARTS], refs[PARTS:]
    join(boxes, x, h)
    ff = gg_ref.shape[1]
    gg_ref[...] = tn(x[...], h[:, :ff]).astype(BF)
    gu_ref[...] = tn(x[...], h[:, ff:]).astype(BF)


def grads_down(t, boxes, rows, ff):
    width = boxes[0].shape[1]
    rows *= PARTS
    return pl.pallas_call(
        grads_down_kernel,
        in_specs=[SMEM] + [VMEM] * PARTS,
        out_specs=[VMEM] * PARTS,
        out_shape=[struct(ff // PARTS, width)] * PARTS,
        scratch_shapes=[pltpu.VMEM((rows, width), BF), pltpu.VMEM((rows, ff), BF)],
        cost_estimate=cost(2 * rows * width * ff, 2 * rows * width * 2),
        compiler_params=pltpu.CompilerParams(vmem_limit_bytes=12 << 20),
        name="grads_down",
    )(t, *boxes)


def grads_up(boxes, rows, ff):
    width = boxes[0].shape[1]
    rows *= PARTS
    return pl.pallas_call(
        grads_up_kernel,
        in_specs=[VMEM] * PARTS,
        out_specs=[VMEM] * 2,
        out_shape=[struct(width, ff)] * 2,
        scratch_shapes=[pltpu.VMEM((rows, width), BF), pltpu.VMEM((rows, 2 * ff), BF)],
        cost_estimate=cost(4 * rows * width * ff, 3 * rows * width * 2),
        compiler_params=pltpu.CompilerParams(vmem_limit_bytes=14 << 20),
        name="grads_up",
    )(*boxes)


def combine_kernel(split, ids_ref, *refs):
    rets, refs = refs[: len(split)], refs[len(split) :]
    out_ref, flats, rhs = refs[0], refs[1 : 1 + len(split)], refs[1 + len(split)]
    n_tok, d = out_ref.shape
    slots = sum(split)
    experts = rets[0].shape[0]
    eighth = d // 8
    blocks = eighth // 128
    lane = lax.broadcasted_iota(jnp.int32, (n_tok, slots * experts), 1)
    expert = lane % experts
    member = jnp.where((ids_ref[:, 0:1] == expert) | (ids_ref[:, 1:2] == expert), 1.0, 0.0).astype(F32)
    i = lax.broadcasted_iota(jnp.int32, (n_tok, n_tok), 0)
    j = lax.broadcasted_iota(jnp.int32, (n_tok, n_tok), 1)
    before = nn(jnp.where(j < i, 1.0, 0.0).astype(BF), member.astype(BF))
    pick = jnp.where(before == (lane // experts).astype(F32), member, 0.0).astype(BF)
    for ret, flat in zip(rets, flats):
        for b in range(flat.shape[0]):
            flat[b] = ret[:, :, b * 128 : (b + 1) * 128].astype(F32).reshape(flat.shape[1:])
    for o in range(8):
        for b in range(blocks):
            col = o * eighth + b * 128
            p = 0
            for flat, count in zip(flats, split):
                for k in range(count):
                    v = flat[k * blocks + b, pl.ds(o, experts, stride=8), :]
                    rhs[p * experts : (p + 1) * experts, col : col + 128] = v.astype(BF)
                    p += 1
    out_ref[...] = nn(pick, rhs[...]).astype(BF)


def combine(ids, rets, split, d):
    n_tok = ids.shape[0]
    slots = sum(split)
    experts = rets[0].shape[0]
    return pl.pallas_call(
        functools.partial(combine_kernel, split),
        in_specs=[VMEM] * (1 + len(split)),
        out_specs=VMEM,
        out_shape=jax.ShapeDtypeStruct((n_tok, d), BF),
        scratch_shapes=[pltpu.VMEM((c * d // 8 // 128, r.shape[0] * 8, 128), F32) for c, r in zip(split, rets)]
        + [pltpu.VMEM((slots * experts, d), BF)],
        cost_estimate=cost(2 * n_tok * slots * experts * d, 4 * n_tok * d * 2),
        compiler_params=pltpu.CompilerParams(vmem_limit_bytes=14 << 20),
        name="combine",
    )(ids, *rets)


def place_kernel(t_ref, *refs):
    out = refs[-1]
    width = refs[0].shape[1]
    for k in range(PARTS):
        at = pl.multiple_of(lax.rem(t_ref[0] - k + PARTS, PARTS) * width, width)
        out[:, pl.ds(at, width)] = refs[k][...]


def place(t, pieces):
    rows, width = pieces[0].shape
    return pl.pallas_call(
        place_kernel,
        in_specs=[SMEM] + [VMEM] * len(pieces),
        out_specs=VMEM,
        out_shape=jax.ShapeDtypeStruct((rows, width * len(pieces)), BF),
        cost_estimate=cost(rows * width, 4 * rows * width * 4),
        compiler_params=pltpu.CompilerParams(vmem_limit_bytes=6 << 20),
        name="place",
    )(t, *pieces)


def local(tokens, cotangent, expert_ids, gate_wts, w_gate, w_up, w_down):
    n_tok, d = tokens.shape
    experts = lax.axis_size("expert")
    slots = 2 * n_tok // experts
    split = (slots,)
    t = lax.axis_index("tensor").astype(jnp.int32).reshape(1)
    ff = w_gate.shape[2]

    def shift(x, k):
        return lax.ppermute(x, "tensor", [(s, (s + k) % PARTS) for s in range(PARTS)])

    def everyone(x):
        return [x] + [shift(x, k) for k in range(1, PARTS)]

    sends = dispatch(expert_ids.T, gate_wts.T, tokens, cotangent, experts, split)
    recvs = []
    for send in sends:
        recvs.append(lax.all_to_all(send, "expert", 0, 0, tiled=True))
    wg, wu, wd = everyone(w_gate[0]), everyone(w_up[0]), everyone(w_down[0])
    wd = stack_down(t, wd)
    (recv,), (count,) = recvs, split
    msg, h = expert_round(t, recv, wg, wu, wd, count)
    rets = [lax.all_to_all(msg, "expert", 0, 0, tiled=True)]
    boxes_c = spread(t, recv, h, 1, 0, ff)
    boxes_c = boxes_c[:1] + [shift(boxes_c[k], k) for k in range(1, PARTS)]
    boxes_x = spread(t, recv, h, 0, ff, 2 * ff)
    boxes_x = boxes_x[:1] + [shift(boxes_x[k], k) for k in range(1, PARTS)]
    down = grads_down(t, boxes_c, h.shape[0], ff)
    down = list(down[:1]) + [shift(down[k], k) for k in range(1, PARTS)]
    grad_gate, grad_up = grads_up(boxes_x, h.shape[0], ff)
    grad_down = place(t, down)
    input_grad = combine(expert_ids, rets, split, d)
    return input_grad, grad_gate[None], grad_up[None], grad_down[None]


def solution(mesh):
    tok = P(("group", "expert", "tensor"), None)
    wts = P("expert", "tensor", None)
    out = P(("group", "expert"), "tensor", None)

    return jax.shard_map(
        local,
        mesh=mesh,
        in_specs=(tok, tok, tok, tok, wts, wts, wts),
        out_specs=(tok, out, out, out),
        check_vma=False,
    )
```

```python
import functools

import jax
import jax.numpy as jnp
from jax import lax
from jax.experimental import pallas as pl
from jax.experimental.pallas import tpu as pltpu
from jax.sharding import PartitionSpec as P


BF = jnp.bfloat16
F32 = jnp.float32
VMEM = pl.BlockSpec(memory_space=pltpu.VMEM)
SMEM = pl.BlockSpec(memory_space=pltpu.SMEM)
HBM = pl.BlockSpec(memory_space=pltpu.HBM)
PARTS = 4
STEPS = 4


def cost(flops, bytes_accessed):
    return pl.CostEstimate(flops=int(flops), bytes_accessed=int(bytes_accessed), transcendentals=0)


def struct(*shape):
    return jax.ShapeDtypeStruct(shape, BF)


def nn(a, b):
    return lax.dot_general(a, b, (((1,), (0,)), ((), ())), preferred_element_type=F32)


def nt(a, b):
    return lax.dot_general(a, b, (((1,), (1,)), ((), ())), preferred_element_type=F32)


def tn(a, b):
    return lax.dot_general(a, b, (((0,), (0,)), ((), ())), preferred_element_type=F32)


def dispatch_kernel(split, ids_ref, gate_ref, *refs):
    sources, refs = refs[:8], refs[8:]
    outs, (pick_ref, scale_ref) = refs[: len(split)], refs[len(split) :]
    n_tok, lanes = sources[0].shape
    experts = outs[0].shape[0]
    rows = experts * 8
    slots = sum(split)

    @pl.when(pl.program_id(0) == 0)
    def _():
        row = lax.broadcasted_iota(jnp.int32, (rows, n_tok), 0)
        expert = row // 8
        first = ids_ref[0:1, :] == expert
        second = ids_ref[1:2, :] == expert
        member = jnp.where(first | second, 1.0, 0.0).astype(F32)
        j = lax.broadcasted_iota(jnp.int32, (n_tok, n_tok), 0)
        i = lax.broadcasted_iota(jnp.int32, (n_tok, n_tok), 1)
        before = nn(member.astype(BF), jnp.where(j < i, 1.0, 0.0).astype(BF))
        gates = jnp.where(first, gate_ref[0:1, :], gate_ref[1:2, :])
        is_cot = row % 2 == 1
        wide = lax.broadcasted_iota(jnp.int32, (rows, 2 * n_tok), 0)
        part = (wide % 8) // 2
        for p in range(slots):
            chosen = jnp.where(before == float(p), member, 0.0)
            weight = jnp.sum(chosen * gates, axis=1, keepdims=True)
            scale_ref[p] = jnp.where(is_cot[:, :1], weight, 1.0)
            kept = jnp.concatenate([jnp.where(is_cot, 0.0, chosen), jnp.where(is_cot, chosen, 0.0)], axis=1)
            for q in range(4):
                pick_ref[p, :, q * 2 * n_tok : (q + 1) * 2 * n_tok] = jnp.where(part == q, kept, 0.0).astype(BF)

    source = jnp.concatenate([s[...] for s in sources], axis=0)
    p = 0
    for out, count in zip(outs, split):
        for k in range(count):
            picked = nn(pick_ref[p], source) * scale_ref[p]
            out[:, :, k * lanes : (k + 1) * lanes] = picked.reshape(experts, 8, lanes).astype(BF)
            p += 1


def dispatch(ids2, gates2, tokens, cotangent, experts, split):
    n_tok, d = tokens.shape
    lanes = d // 4 // STEPS
    rows = experts * 8
    slots = sum(split)
    columns = []
    for q in range(4):
        columns += [pl.BlockSpec((n_tok, lanes), lambda i, q=q: (0, q * STEPS + i))] * 2
    return pl.pallas_call(
        functools.partial(dispatch_kernel, split),
        grid=(STEPS,),
        in_specs=[pl.BlockSpec((2, n_tok), lambda i: (0, 0))] * 2 + columns,
        out_specs=[pl.BlockSpec((experts, 8, c * lanes), lambda i: (0, 0, i)) for c in split],
        out_shape=[jax.ShapeDtypeStruct((experts, 8, c * d // 4), BF) for c in split],
        scratch_shapes=[pltpu.VMEM((slots, rows, 8 * n_tok), BF), pltpu.VMEM((slots, rows, 1), F32)],
        cost_estimate=cost(2 * slots * rows * 8 * n_tok * d // 4, 4 * n_tok * d * 2 + 2 * slots * experts * d * 2),
        name="dispatch",
    )(ids2, gates2, *([tokens, cotangent] * 4))


def stack_kernel(t_ref, *refs):
    out = refs[-1]
    part = refs[0].shape[0]
    for k in range(PARTS):
        at = pl.multiple_of(lax.rem(t_ref[0] - k + PARTS, PARTS) * part, part)
        out[pl.ds(at, part), :] = refs[k][...]


def stack_down(t, pieces):
    part, d = pieces[0].shape
    return pl.pallas_call(
        stack_kernel,
        in_specs=[SMEM] + [VMEM] * PARTS,
        out_specs=VMEM,
        out_shape=jax.ShapeDtypeStruct((part * PARTS, d), BF),
        cost_estimate=cost(part * d, 4 * part * d * 4),
        name="stack_down",
    )(t, *pieces)


def unpack(block, flat, step, kinds):
    sources = block.shape[0]
    d = kinds[0][1].shape[1]
    count = kinds[0][1].shape[0] // sources
    lanes = d // 4 // STEPS
    blocks = lanes // 128
    for b in range(flat.shape[0]):
        flat[b] = block[:, :, b * 128 : (b + 1) * 128].astype(F32).reshape(flat.shape[1:])
    for p in range(count):
        for b in range(blocks):
            for q in range(4):
                col = q * (d // 4) + step * lanes + b * 128
                for kind, dst in kinds:
                    v = flat[p * blocks + b, pl.ds(2 * q + kind, sources, stride=8), :]
                    dst[p * sources : (p + 1) * sources, col : col + 128] = v.astype(BF)


def flat_scratch(recv):
    return pltpu.VMEM((STEPS, recv.shape[2] // STEPS // 128, recv.shape[0] * 8, 128), F32)


def expert_kernel(count, t_ref, recv_ref, *refs):
    weights, refs = refs[: 2 * PARTS + 1], refs[2 * PARTS + 1 :]
    msg_ref, h_ref, flat, x, c, back, ret, msg = refs[:8]
    held, sem_out, sem_w = refs[8 : 8 + len(weights)], refs[-2], refs[-1]
    wg, wu, wd = held[:PARTS], held[PARTS : 2 * PARTS], held[2 * PARTS]
    t = t_ref[0]
    width, ff = wg[0].shape
    d = wd.shape[1]
    sources = recv_ref.shape[0]
    lanes = recv_ref.shape[2] // STEPS
    weights_in = [pltpu.make_async_copy(w, v, sem_w.at[i]) for i, (w, v) in enumerate(zip(weights, held))]
    for copy in weights_in:
        copy.start()
    for i in range(STEPS):
        unpack(recv_ref.at[:, :, pl.ds(i * lanes, lanes)], flat.at[i], i, [(0, x), (1, c)])
    for copy in weights_in:
        copy.wait()
    cols = [pl.ds(pl.multiple_of(lax.rem(t - k + PARTS, PARTS) * width, width), width) for k in range(PARTS)]
    pre_gate = functools.reduce(lambda a, b: a + b, [nn(x[:, cols[k]], wg[k][...]) for k in range(PARTS)])
    pre_up = functools.reduce(lambda a, b: a + b, [nn(x[:, cols[k]], wu[k][...]) for k in range(PARTS)])
    grad_hidden = nt(c[...], wd[...])
    sig = jax.nn.sigmoid(pre_gate)
    activated = pre_gate * sig
    grad_gate_pre = (grad_hidden * pre_up * sig * (1.0 + pre_gate * (1.0 - sig))).astype(BF)
    grad_up_pre = (grad_hidden * activated).astype(BF)
    hidden = (activated * pre_up).astype(BF)
    for k in range(PARTS):
        back[:, cols[k]] = nt(grad_gate_pre, wg[k][...]) + nt(grad_up_pre, wu[k][...])
    eighth = d // 8
    blocks = eighth // 128
    out = [
        pltpu.make_async_copy(msg.at[p], msg_ref.at[:, :, pl.ds(p * eighth, eighth)], sem_out.at[p]) for p in range(count)
    ]
    for p in range(count):
        for b in range(blocks):
            for o in range(8):
                col = o * eighth + b * 128
                ret[p * blocks + b, pl.ds(o, sources, stride=8), :] = back[p * sources : (p + 1) * sources, col : col + 128]
        for b in range(blocks):
            msg[p, :, :, b * 128 : (b + 1) * 128] = ret[p * blocks + b].reshape(sources, 8, 128).astype(BF)
        if p:
            out[p - 1].start()
    h_ref[:, 0:ff] = hidden
    h_ref[:, ff : 2 * ff] = grad_gate_pre
    h_ref[:, 2 * ff :] = grad_up_pre
    out[-1].start()
    for copy in out:
        copy.wait()


def expert_round(t, recv, wg, wu, wd, count):
    sources = recv.shape[0]
    ff, d = wd.shape
    rows = sources * count
    return pl.pallas_call(
        functools.partial(expert_kernel, count),
        in_specs=[SMEM, VMEM] + [HBM] * (1 + 2 * PARTS),
        out_specs=[HBM, VMEM],
        out_shape=[struct(sources, 8, count * d // 8), struct(rows, 3 * ff)],
        scratch_shapes=[
            flat_scratch(recv),
            pltpu.VMEM((rows, d), BF),
            pltpu.VMEM((rows, d), BF),
            pltpu.VMEM((rows, d), F32),
            pltpu.VMEM((count * d // 8 // 128, sources * 8, 128), F32),
            pltpu.VMEM((count, sources, 8, d // 8), BF),
        ]
        + [pltpu.VMEM(w.shape, BF) for w in (*wg, *wu, wd)]
        + [pltpu.SemaphoreType.DMA((count,)), pltpu.SemaphoreType.DMA((2 * PARTS + 1,))],
        cost_estimate=cost(2 * rows * d * 5 * ff, 3 * ff * d * 2 + 3 * rows * d * 2),
        compiler_params=pltpu.CompilerParams(vmem_limit_bytes=60 << 20),
        name="expert_round",
    )(t, recv, *wg, *wu, wd)


def spread_kernel(kind, first, wide, t_ref, recv_ref, h_ref, *refs):
    boxes, (flat, x) = refs[:PARTS], refs[PARTS:]
    lanes = recv_ref.shape[2] // STEPS
    for i in range(STEPS):
        unpack(recv_ref.at[:, :, pl.ds(i * lanes, lanes)], flat.at[i], i, [(kind, x)])
    rows, d = x.shape
    width = d // PARTS
    folds = width // wide
    part = rows // folds
    for k in range(PARTS):
        there = pl.ds(pl.multiple_of(lax.rem(t_ref[0] + k, PARTS) * width, width), width)
        boxes[k][0:rows, :] = x[:, there]
        for f in range(folds):
            boxes[k][rows:, f * wide : (f + 1) * wide] = h_ref[f * part : (f + 1) * part, first : first + wide]


def spread(t, recv, h, kind, first, wide):
    rows = h.shape[0]
    d = recv.shape[2] * 8 * recv.shape[0] // (2 * rows)
    width = d // PARTS
    return list(
        pl.pallas_call(
            functools.partial(spread_kernel, kind, first, wide),
            in_specs=[SMEM] + [VMEM] * 2,
            out_specs=[VMEM] * PARTS,
            out_shape=[struct(rows + rows * wide // width, width)] * PARTS,
            scratch_shapes=[flat_scratch(recv), pltpu.VMEM((rows, d), BF)],
            cost_estimate=cost(rows * d, 6 * rows * d),
            compiler_params=pltpu.CompilerParams(vmem_limit_bytes=60 << 20),
        )(t, recv, h)
    )


def join(boxes, x, h):
    rows = x.shape[0] // len(boxes)
    wide = h.shape[1]
    folds = x.shape[1] // wide
    part = rows // folds
    for i, box in enumerate(boxes):
        x[i * rows : (i + 1) * rows, :] = box[0:rows, :]
        for f in range(folds):
            h[i * rows + f * part : i * rows + (f + 1) * part, :] = box[rows:, f * wide : (f + 1) * wide]


def grads_down_kernel(t_ref, *refs):
    boxes, downs, (c, h) = refs[:PARTS], refs[PARTS : 2 * PARTS], refs[2 * PARTS :]
    join(boxes, c, h)
    ff = h.shape[1]
    c[0:ff, :] = tn(h[...], c[...]).astype(BF)
    part = ff // PARTS
    for k in range(PARTS):
        downs[k][...] = c[pl.ds(pl.multiple_of(lax.rem(t_ref[0] + k, PARTS) * part, part), part), :]


def grads_up_kernel(*refs):
    boxes, (gg_ref, gu_ref, x, h) = refs[:PARTS], refs[PARTS:]
    join(boxes, x, h)
    ff = gg_ref.shape[1]
    gg_ref[...] = tn(x[...], h[:, :ff]).astype(BF)
    gu_ref[...] = tn(x[...], h[:, ff:]).astype(BF)


def grads_down(t, boxes, rows, ff):
    width = boxes[0].shape[1]
    rows *= PARTS
    return pl.pallas_call(
        grads_down_kernel,
        in_specs=[SMEM] + [VMEM] * PARTS,
        out_specs=[VMEM] * PARTS,
        out_shape=[struct(ff // PARTS, width)] * PARTS,
        scratch_shapes=[pltpu.VMEM((rows, width), BF), pltpu.VMEM((rows, ff), BF)],
        cost_estimate=cost(2 * rows * width * ff, 2 * rows * width * 2),
        name="grads_down",
    )(t, *boxes)


def grads_up(boxes, rows, ff):
    width = boxes[0].shape[1]
    rows *= PARTS
    return pl.pallas_call(
        grads_up_kernel,
        in_specs=[VMEM] * PARTS,
        out_specs=[VMEM] * 2,
        out_shape=[struct(width, ff)] * 2,
        scratch_shapes=[pltpu.VMEM((rows, width), BF), pltpu.VMEM((rows, 2 * ff), BF)],
        cost_estimate=cost(4 * rows * width * ff, 3 * rows * width * 2),
        name="grads_up",
    )(*boxes)


def combine_kernel(split, ids_ref, *refs):
    rets, refs = refs[: len(split)], refs[len(split) :]
    out_ref, flats, rhs = refs[0], refs[1 : 1 + len(split)], refs[1 + len(split)]
    n_tok, d = out_ref.shape
    slots = sum(split)
    experts = rets[0].shape[0]
    eighth = d // 8
    blocks = eighth // 128
    lane = lax.broadcasted_iota(jnp.int32, (n_tok, slots * experts), 1)
    expert = lane % experts
    member = jnp.where((ids_ref[:, 0:1] == expert) | (ids_ref[:, 1:2] == expert), 1.0, 0.0).astype(F32)
    i = lax.broadcasted_iota(jnp.int32, (n_tok, n_tok), 0)
    j = lax.broadcasted_iota(jnp.int32, (n_tok, n_tok), 1)
    before = nn(jnp.where(j < i, 1.0, 0.0).astype(BF), member.astype(BF))
    pick = jnp.where(before == (lane // experts).astype(F32), member, 0.0).astype(BF)
    for ret, flat in zip(rets, flats):
        for b in range(flat.shape[0]):
            flat[b] = ret[:, :, b * 128 : (b + 1) * 128].astype(F32).reshape(flat.shape[1:])
    for o in range(8):
        for b in range(blocks):
            col = o * eighth + b * 128
            p = 0
            for flat, count in zip(flats, split):
                for k in range(count):
                    v = flat[k * blocks + b, pl.ds(o, experts, stride=8), :]
                    rhs[p * experts : (p + 1) * experts, col : col + 128] = v.astype(BF)
                    p += 1
    out_ref[...] = nn(pick, rhs[...]).astype(BF)


def combine(ids, rets, split, d):
    n_tok = ids.shape[0]
    slots = sum(split)
    experts = rets[0].shape[0]
    return pl.pallas_call(
        functools.partial(combine_kernel, split),
        in_specs=[VMEM] * (1 + len(split)),
        out_specs=VMEM,
        out_shape=jax.ShapeDtypeStruct((n_tok, d), BF),
        scratch_shapes=[pltpu.VMEM((c * d // 8 // 128, r.shape[0] * 8, 128), F32) for c, r in zip(split, rets)]
        + [pltpu.VMEM((slots * experts, d), BF)],
        cost_estimate=cost(2 * n_tok * slots * experts * d, 4 * n_tok * d * 2),
        compiler_params=pltpu.CompilerParams(vmem_limit_bytes=14 << 20),
        name="combine",
    )(ids, *rets)


def place_kernel(t_ref, *refs):
    out = refs[-1]
    width = refs[0].shape[1]
    for k in range(PARTS):
        at = pl.multiple_of(lax.rem(t_ref[0] - k + PARTS, PARTS) * width, width)
        out[:, pl.ds(at, width)] = refs[k][...]


def place(t, pieces):
    rows, width = pieces[0].shape
    return pl.pallas_call(
        place_kernel,
        in_specs=[SMEM] + [VMEM] * len(pieces),
        out_specs=VMEM,
        out_shape=jax.ShapeDtypeStruct((rows, width * len(pieces)), BF),
        cost_estimate=cost(rows * width, 4 * rows * width * 4),
        name="place",
    )(t, *pieces)


def local(tokens, cotangent, expert_ids, gate_wts, w_gate, w_up, w_down):
    n_tok, d = tokens.shape
    experts = lax.axis_size("expert")
    slots = 2 * n_tok // experts
    split = (slots,)
    t = lax.axis_index("tensor").astype(jnp.int32).reshape(1)
    ff = w_gate.shape[2]

    def shift(x, k):
        return lax.ppermute(x, "tensor", [(s, (s + k) % PARTS) for s in range(PARTS)])

    def everyone(x):
        return [x] + [shift(x, k) for k in range(1, PARTS)]

    sends = dispatch(expert_ids.T, gate_wts.T, tokens, cotangent, experts, split)
    recvs = []
    for send in sends:
        recvs.append(lax.all_to_all(send, "expert", 0, 0, tiled=True))
    wg, wu, wd = everyone(w_gate[0]), everyone(w_up[0]), everyone(w_down[0])
    wd = stack_down(t, wd)
    (recv,), (count,) = recvs, split
    msg, h = expert_round(t, recv, wg, wu, wd, count)
    rets = [lax.all_to_all(msg, "expert", 0, 0, tiled=True)]
    boxes_c = spread(t, recv, h, 1, 0, ff)
    boxes_c = boxes_c[:1] + [shift(boxes_c[k], k) for k in range(1, PARTS)]
    boxes_x = spread(t, recv, h, 0, ff, 2 * ff)
    boxes_x = boxes_x[:1] + [shift(boxes_x[k], k) for k in range(1, PARTS)]
    down = grads_down(t, boxes_c, h.shape[0], ff)
    down = list(down[:1]) + [shift(down[k], k) for k in range(1, PARTS)]
    grad_gate, grad_up = grads_up(boxes_x, h.shape[0], ff)
    grad_down = place(t, down)
    input_grad = combine(expert_ids, rets, split, d)
    return input_grad, grad_gate[None], grad_up[None], grad_down[None]


def solution(mesh):
    tok = P(("group", "expert", "tensor"), None)
    wts = P("expert", "tensor", None)
    out = P(("group", "expert"), "tensor", None)

    return jax.shard_map(
        local,
        mesh=mesh,
        in_specs=(tok, tok, tok, tok, wts, wts, wts),
        out_specs=(tok, out, out, out),
        check_vma=False,
    )
```

```python
import functools

import jax
import jax.numpy as jnp
from jax import lax
from jax.experimental import pallas as pl
from jax.experimental.pallas import tpu as pltpu
from jax.sharding import PartitionSpec as P


BF = jnp.bfloat16
F32 = jnp.float32
VMEM = pl.BlockSpec(memory_space=pltpu.VMEM)
SMEM = pl.BlockSpec(memory_space=pltpu.SMEM)
HBM = pl.BlockSpec(memory_space=pltpu.HBM)
PARTS = 4
STEPS = 4


def cost(flops, bytes_accessed):
    return pl.CostEstimate(flops=int(flops), bytes_accessed=int(bytes_accessed), transcendentals=0)


def struct(*shape):
    return jax.ShapeDtypeStruct(shape, BF)


def nn(a, b):
    return lax.dot_general(a, b, (((1,), (0,)), ((), ())), preferred_element_type=F32)


def nt(a, b):
    return lax.dot_general(a, b, (((1,), (1,)), ((), ())), preferred_element_type=F32)


def tn(a, b):
    return lax.dot_general(a, b, (((0,), (0,)), ((), ())), preferred_element_type=F32)


def dispatch_kernel(split, ids_ref, gate_ref, *refs):
    sources, refs = refs[:8], refs[8:]
    outs, (pick_ref, scale_ref) = refs[: len(split)], refs[len(split) :]
    n_tok, lanes = sources[0].shape
    experts = outs[0].shape[0]
    rows = experts * 8
    slots = sum(split)

    @pl.when(pl.program_id(0) == 0)
    def _():
        row = lax.broadcasted_iota(jnp.int32, (rows, n_tok), 0)
        expert = row // 8
        first = ids_ref[0:1, :] == expert
        second = ids_ref[1:2, :] == expert
        member = jnp.where(first | second, 1.0, 0.0).astype(F32)
        j = lax.broadcasted_iota(jnp.int32, (n_tok, n_tok), 0)
        i = lax.broadcasted_iota(jnp.int32, (n_tok, n_tok), 1)
        before = nn(member.astype(BF), jnp.where(j < i, 1.0, 0.0).astype(BF))
        gates = jnp.where(first, gate_ref[0:1, :], gate_ref[1:2, :])
        is_cot = row % 2 == 1
        wide = lax.broadcasted_iota(jnp.int32, (rows, 2 * n_tok), 0)
        part = (wide % 8) // 2
        for p in range(slots):
            chosen = jnp.where(before == float(p), member, 0.0)
            weight = jnp.sum(chosen * gates, axis=1, keepdims=True)
            scale_ref[p] = jnp.where(is_cot[:, :1], weight, 1.0)
            kept = jnp.concatenate([jnp.where(is_cot, 0.0, chosen), jnp.where(is_cot, chosen, 0.0)], axis=1)
            for q in range(4):
                pick_ref[p, :, q * 2 * n_tok : (q + 1) * 2 * n_tok] = jnp.where(part == q, kept, 0.0).astype(BF)

    source = jnp.concatenate([s[...] for s in sources], axis=0)
    p = 0
    for out, count in zip(outs, split):
        for k in range(count):
            picked = nn(pick_ref[p], source) * scale_ref[p]
            out[:, :, k * lanes : (k + 1) * lanes] = picked.reshape(experts, 8, lanes).astype(BF)
            p += 1


def dispatch(ids2, gates2, tokens, cotangent, experts, split):
    n_tok, d = tokens.shape
    lanes = d // 4 // STEPS
    rows = experts * 8
    slots = sum(split)
    columns = []
    for q in range(4):
        columns += [pl.BlockSpec((n_tok, lanes), lambda i, q=q: (0, q * STEPS + i))] * 2
    return pl.pallas_call(
        functools.partial(dispatch_kernel, split),
        grid=(STEPS,),
        in_specs=[pl.BlockSpec((2, n_tok), lambda i: (0, 0))] * 2 + columns,
        out_specs=[pl.BlockSpec((experts, 8, c * lanes), lambda i: (0, 0, i)) for c in split],
        out_shape=[jax.ShapeDtypeStruct((experts, 8, c * d // 4), BF) for c in split],
        scratch_shapes=[pltpu.VMEM((slots, rows, 8 * n_tok), BF), pltpu.VMEM((slots, rows, 1), F32)],
        cost_estimate=cost(2 * slots * rows * 8 * n_tok * d // 4, 4 * n_tok * d * 2 + 2 * slots * experts * d * 2),
        name="dispatch",
    )(ids2, gates2, *([tokens, cotangent] * 4))


def stack_kernel(at_ref, *refs):
    wg, wu, wd, out = refs[:PARTS], refs[PARTS : 2 * PARTS], refs[2 * PARTS : 3 * PARTS], refs[-1]
    width, ff = wg[0].shape
    part, d = wd[0].shape
    for k in range(PARTS):
        owner = lax.rem(at_ref[0] - k + PARTS, PARTS)
        rows = pl.ds(pl.multiple_of(owner * width, width), width)
        out[rows, 0:ff] = wg[k][...]
        out[rows, ff:] = wu[k][...]
        for b in range(d // (2 * ff)):
            at = pl.multiple_of(d + b * ff + owner * part, part)
            out[pl.ds(at, part), :] = wd[k][:, b * 2 * ff : (b + 1) * 2 * ff]


def stack(t, wg, wu, wd):
    _, ff = wg[0].shape
    d = wd[0].shape[1]
    return pl.pallas_call(
        stack_kernel,
        in_specs=[SMEM] + [VMEM] * (3 * PARTS),
        out_specs=VMEM,
        out_shape=struct(d + d // 2, 2 * ff),
        cost_estimate=cost(3 * d * ff, 12 * d * ff),
        name="stack",
    )(t, *wg, *wu, *wd)


def widen(recv_ref, flat):
    for b in range(flat.shape[0]):
        flat[b] = recv_ref[:, :, b * 128 : (b + 1) * 128].astype(F32).reshape(flat.shape[1:])


def unpack(flat, sources, q, kinds):
    d = kinds[0][1].shape[1]
    count = kinds[0][1].shape[0] // sources
    lanes = d // 4 // STEPS
    blocks = lanes // 128
    for step in range(STEPS):
        for p in range(count):
            for b in range(blocks):
                col = q * (d // 4) + step * lanes + b * 128
                for kind, dst in kinds:
                    v = flat[(step * count + p) * blocks + b, pl.ds(2 * q + kind, sources, stride=8), :]
                    dst[p * sources : (p + 1) * sources, col : col + 128] = v.astype(BF)


def flat_scratch(recv):
    return pltpu.VMEM((recv.shape[2] // 128, recv.shape[0] * 8, 128), F32)


def expert_kernel(count, recv_ref, w_ref, msg_ref, h_ref, flat, x, c, back, ret, wgu, wd, sem_w):
    sources = recv_ref.shape[0]
    d = x.shape[1]
    width = d // 4
    ff = wgu.shape[1] // 2
    weights_in = [
        pltpu.make_async_copy(
            w_ref.at[pl.ds(q * width, width), :], wgu.at[pl.ds(q * width, width), :], sem_w.at[q]
        )
        for q in range(4)
    ] + [pltpu.make_async_copy(w_ref.at[pl.ds(d, d // 2), :], wd, sem_w.at[4])]
    for copy in weights_in:
        copy.start()
    widen(recv_ref, flat)
    pre = jnp.zeros((x.shape[0], 2 * ff), F32)
    for q in range(4):
        unpack(flat, sources, q, [(0, x), (1, c)])
        weights_in[q].wait()
        cols = slice(q * width, (q + 1) * width)
        pre += nn(x[:, cols], wgu[cols, :])
    weights_in[4].wait()
    grad_hidden = jnp.zeros((x.shape[0], ff), F32)
    for b in range(d // (2 * ff)):
        grad_hidden += nt(c[:, b * 2 * ff : (b + 1) * 2 * ff], wd[b * ff : (b + 1) * ff, :])
    pre_gate, pre_up = pre[:, :ff], pre[:, ff:]
    sig = jax.nn.sigmoid(pre_gate)
    activated = pre_gate * sig
    grad_gate_pre = (grad_hidden * pre_up * sig * (1.0 + pre_gate * (1.0 - sig))).astype(BF)
    grad_up_pre = (grad_hidden * activated).astype(BF)
    hidden = (activated * pre_up).astype(BF)
    both = jnp.concatenate([grad_gate_pre, grad_up_pre], axis=1)
    for q in range(4):
        cols = slice(q * width, (q + 1) * width)
        back[:, cols] = nt(both, wgu[cols, :])
    eighth = d // 8
    blocks = eighth // 128
    for p in range(count):
        for b in range(blocks):
            for o in range(8):
                col = o * eighth + b * 128
                ret[p * blocks + b, pl.ds(o, sources, stride=8), :] = back[p * sources : (p + 1) * sources, col : col + 128]
        for b in range(blocks):
            at = p * eighth + b * 128
            msg_ref[:, :, at : at + 128] = ret[p * blocks + b].reshape(sources, 8, 128).astype(BF)
    h_ref[:, 0:ff] = hidden
    h_ref[:, ff:] = both


def expert_round(recv, weights, ff, count):
    sources = recv.shape[0]
    d = recv.shape[2] * 4 // count
    rows = sources * count
    return pl.pallas_call(
        functools.partial(expert_kernel, count),
        in_specs=[VMEM, HBM],
        out_specs=[VMEM] * 2,
        out_shape=[struct(sources, 8, count * d // 8), struct(rows, 3 * ff)],
        scratch_shapes=[
            flat_scratch(recv),
            pltpu.VMEM((rows, d), BF),
            pltpu.VMEM((rows, d), BF),
            pltpu.VMEM((rows, d), F32),
            pltpu.VMEM((count * d // 8 // 128, sources * 8, 128), F32),
            pltpu.VMEM((d, 2 * ff), BF),
            pltpu.VMEM((d // 2, 2 * ff), BF),
            pltpu.SemaphoreType.DMA((5,)),
        ],
        cost_estimate=cost(2 * rows * d * 5 * ff, 3 * ff * d * 2 + 3 * rows * d * 2),
        compiler_params=pltpu.CompilerParams(vmem_limit_bytes=50 << 20),
        name="expert_round",
    )(recv, weights)


def spread_kernel(kind, first, wide, t_ref, recv_ref, h_ref, *refs):
    boxes, (flat, x) = refs[:PARTS], refs[PARTS:]
    widen(recv_ref, flat)
    for q in range(4):
        unpack(flat, recv_ref.shape[0], q, [(kind, x)])
    rows, d = x.shape
    width = d // PARTS
    folds = width // wide
    part = rows // folds
    for k in range(PARTS):
        there = pl.ds(pl.multiple_of(lax.rem(t_ref[0] + k, PARTS) * width, width), width)
        boxes[k][0:rows, :] = x[:, there]
        for f in range(folds):
            boxes[k][rows:, f * wide : (f + 1) * wide] = h_ref[f * part : (f + 1) * part, first : first + wide]


def spread(t, recv, h, kind, first, wide):
    rows = h.shape[0]
    d = recv.shape[2] * 8 * recv.shape[0] // (2 * rows)
    width = d // PARTS
    return list(
        pl.pallas_call(
            functools.partial(spread_kernel, kind, first, wide),
            in_specs=[SMEM] + [VMEM] * 2,
            out_specs=[VMEM] * PARTS,
            out_shape=[struct(rows + rows * wide // width, width)] * PARTS,
            scratch_shapes=[flat_scratch(recv), pltpu.VMEM((rows, d), BF)],
            cost_estimate=cost(rows * d, 6 * rows * d),
            compiler_params=pltpu.CompilerParams(vmem_limit_bytes=50 << 20),
        )(t, recv, h)
    )


def join(boxes, x, h):
    rows = x.shape[0] // len(boxes)
    wide = h.shape[1]
    folds = x.shape[1] // wide
    part = rows // folds
    for i, box in enumerate(boxes):
        x[i * rows : (i + 1) * rows, :] = box[0:rows, :]
        for f in range(folds):
            h[i * rows + f * part : i * rows + (f + 1) * part, :] = box[rows:, f * wide : (f + 1) * wide]


def grads_down_kernel(t_ref, *refs):
    boxes, downs, (c, h) = refs[:PARTS], refs[PARTS : 2 * PARTS], refs[2 * PARTS :]
    join(boxes, c, h)
    ff = h.shape[1]
    c[0:ff, :] = tn(h[...], c[...]).astype(BF)
    part = ff // PARTS
    for k in range(PARTS):
        downs[k][...] = c[pl.ds(pl.multiple_of(lax.rem(t_ref[0] + k, PARTS) * part, part), part), :]


def grads_up_kernel(*refs):
    boxes, (gg_ref, gu_ref, x, h) = refs[:PARTS], refs[PARTS:]
    join(boxes, x, h)
    ff = gg_ref.shape[1]
    gg_ref[...] = tn(x[...], h[:, :ff]).astype(BF)
    gu_ref[...] = tn(x[...], h[:, ff:]).astype(BF)


def grads_down(t, boxes, rows, ff):
    width = boxes[0].shape[1]
    rows *= PARTS
    return pl.pallas_call(
        grads_down_kernel,
        in_specs=[SMEM] + [VMEM] * PARTS,
        out_specs=[VMEM] * PARTS,
        out_shape=[struct(ff // PARTS, width)] * PARTS,
        scratch_shapes=[pltpu.VMEM((rows, width), BF), pltpu.VMEM((rows, ff), BF)],
        cost_estimate=cost(2 * rows * width * ff, 2 * rows * width * 2),
        name="grads_down",
    )(t, *boxes)


def grads_up(boxes, rows, ff):
    width = boxes[0].shape[1]
    rows *= PARTS
    return pl.pallas_call(
        grads_up_kernel,
        in_specs=[VMEM] * PARTS,
        out_specs=[VMEM] * 2,
        out_shape=[struct(width, ff)] * 2,
        scratch_shapes=[pltpu.VMEM((rows, width), BF), pltpu.VMEM((rows, 2 * ff), BF)],
        cost_estimate=cost(4 * rows * width * ff, 3 * rows * width * 2),
        name="grads_up",
    )(*boxes)


def combine_kernel(split, ids_ref, *refs):
    rets, refs = refs[: len(split)], refs[len(split) :]
    out_ref, flats, rhs = refs[0], refs[1 : 1 + len(split)], refs[1 + len(split)]
    n_tok, d = out_ref.shape
    slots = sum(split)
    experts = rets[0].shape[0]
    eighth = d // 8
    blocks = eighth // 128
    lane = lax.broadcasted_iota(jnp.int32, (n_tok, slots * experts), 1)
    expert = lane % experts
    member = jnp.where((ids_ref[:, 0:1] == expert) | (ids_ref[:, 1:2] == expert), 1.0, 0.0).astype(F32)
    i = lax.broadcasted_iota(jnp.int32, (n_tok, n_tok), 0)
    j = lax.broadcasted_iota(jnp.int32, (n_tok, n_tok), 1)
    before = nn(jnp.where(j < i, 1.0, 0.0).astype(BF), member.astype(BF))
    pick = jnp.where(before == (lane // experts).astype(F32), member, 0.0).astype(BF)
    for ret, flat in zip(rets, flats):
        for b in range(flat.shape[0]):
            flat[b] = ret[:, :, b * 128 : (b + 1) * 128].astype(F32).reshape(flat.shape[1:])
    for o in range(8):
        for b in range(blocks):
            col = o * eighth + b * 128
            p = 0
            for flat, count in zip(flats, split):
                for k in range(count):
                    v = flat[k * blocks + b, pl.ds(o, experts, stride=8), :]
                    rhs[p * experts : (p + 1) * experts, col : col + 128] = v.astype(BF)
                    p += 1
    out_ref[...] = nn(pick, rhs[...]).astype(BF)


def combine(ids, rets, split, d):
    n_tok = ids.shape[0]
    slots = sum(split)
    experts = rets[0].shape[0]
    return pl.pallas_call(
        functools.partial(combine_kernel, split),
        in_specs=[VMEM] * (1 + len(split)),
        out_specs=VMEM,
        out_shape=jax.ShapeDtypeStruct((n_tok, d), BF),
        scratch_shapes=[pltpu.VMEM((c * d // 8 // 128, r.shape[0] * 8, 128), F32) for c, r in zip(split, rets)]
        + [pltpu.VMEM((slots * experts, d), BF)],
        cost_estimate=cost(2 * n_tok * slots * experts * d, 4 * n_tok * d * 2),
        compiler_params=pltpu.CompilerParams(vmem_limit_bytes=14 << 20),
        name="combine",
    )(ids, *rets)


def place_kernel(t_ref, *refs):
    out = refs[-1]
    width = refs[0].shape[1]
    for k in range(PARTS):
        at = pl.multiple_of(lax.rem(t_ref[0] - k + PARTS, PARTS) * width, width)
        out[:, pl.ds(at, width)] = refs[k][...]


def place(t, pieces):
    rows, width = pieces[0].shape
    return pl.pallas_call(
        place_kernel,
        in_specs=[SMEM] + [VMEM] * len(pieces),
        out_specs=VMEM,
        out_shape=jax.ShapeDtypeStruct((rows, width * len(pieces)), BF),
        cost_estimate=cost(rows * width, 4 * rows * width * 4),
        name="place",
    )(t, *pieces)


def local(tokens, cotangent, expert_ids, gate_wts, w_gate, w_up, w_down):
    n_tok, d = tokens.shape
    experts = lax.axis_size("expert")
    slots = 2 * n_tok // experts
    split = (slots,)
    t = lax.axis_index("tensor").astype(jnp.int32).reshape(1)
    ff = w_gate.shape[2]

    def shift(x, k):
        return lax.ppermute(x, "tensor", [(s, (s + k) % PARTS) for s in range(PARTS)])

    def everyone(x):
        return [x] + [shift(x, k) for k in range(1, PARTS)]

    sends = dispatch(expert_ids.T, gate_wts.T, tokens, cotangent, experts, split)
    recvs = []
    for send in sends:
        recvs.append(lax.all_to_all(send, "expert", 0, 0, tiled=True))
    wg, wu, wd = everyone(w_gate[0]), everyone(w_up[0]), everyone(w_down[0])
    weights = stack(t, wg, wu, wd)
    (recv,), (count,) = recvs, split
    msg, h = expert_round(recv, weights, ff, count)
    rets = [lax.all_to_all(msg, "expert", 0, 0, tiled=True)]
    boxes_c = spread(t, recv, h, 1, 0, ff)
    boxes_c = boxes_c[:1] + [shift(boxes_c[k], k) for k in range(1, PARTS)]
    boxes_x = spread(t, recv, h, 0, ff, 2 * ff)
    boxes_x = boxes_x[:1] + [shift(boxes_x[k], k) for k in range(1, PARTS)]
    down = grads_down(t, boxes_c, h.shape[0], ff)
    down = list(down[:1]) + [shift(down[k], k) for k in range(1, PARTS)]
    grad_gate, grad_up = grads_up(boxes_x, h.shape[0], ff)
    grad_down = place(t, down)
    input_grad = combine(expert_ids, rets, split, d)
    return input_grad, grad_gate[None], grad_up[None], grad_down[None]


def solution(mesh):
    tok = P(("group", "expert", "tensor"), None)
    wts = P("expert", "tensor", None)
    out = P(("group", "expert"), "tensor", None)

    return jax.shard_map(
        local,
        mesh=mesh,
        in_specs=(tok, tok, tok, tok, wts, wts, wts),
        out_specs=(tok, out, out, out),
        check_vma=False,
    )
```

```python
import functools

import jax
import jax.numpy as jnp
from jax import lax
from jax.experimental import pallas as pl
from jax.experimental.pallas import tpu as pltpu
from jax.sharding import PartitionSpec as P


BF = jnp.bfloat16
F32 = jnp.float32
VMEM = pl.BlockSpec(memory_space=pltpu.VMEM)
SMEM = pl.BlockSpec(memory_space=pltpu.SMEM)
HBM = pl.BlockSpec(memory_space=pltpu.HBM)
PARTS = 4
STEPS = 2


def cost(flops, bytes_accessed):
    return pl.CostEstimate(flops=int(flops), bytes_accessed=int(bytes_accessed), transcendentals=0)


def struct(*shape):
    return jax.ShapeDtypeStruct(shape, BF)


def nn(a, b):
    return lax.dot_general(a, b, (((1,), (0,)), ((), ())), preferred_element_type=F32)


def nt(a, b):
    return lax.dot_general(a, b, (((1,), (1,)), ((), ())), preferred_element_type=F32)


def tn(a, b):
    return lax.dot_general(a, b, (((0,), (0,)), ((), ())), preferred_element_type=F32)


def dispatch_kernel(split, ids_ref, gate_ref, *refs):
    sources, refs = refs[:8], refs[8:]
    outs, (pick_ref, scale_ref) = refs[: len(split)], refs[len(split) :]
    n_tok, lanes = sources[0].shape
    experts = outs[0].shape[0]
    rows = experts * 8
    slots = sum(split)

    @pl.when(pl.program_id(0) == 0)
    def _():
        row = lax.broadcasted_iota(jnp.int32, (rows, n_tok), 0)
        expert = row // 8
        first = ids_ref[0:1, :] == expert
        second = ids_ref[1:2, :] == expert
        member = jnp.where(first | second, 1.0, 0.0).astype(F32)
        j = lax.broadcasted_iota(jnp.int32, (n_tok, n_tok), 0)
        i = lax.broadcasted_iota(jnp.int32, (n_tok, n_tok), 1)
        before = nn(member.astype(BF), jnp.where(j < i, 1.0, 0.0).astype(BF))
        gates = jnp.where(first, gate_ref[0:1, :], gate_ref[1:2, :])
        is_cot = row % 2 == 1
        wide = lax.broadcasted_iota(jnp.int32, (rows, 2 * n_tok), 0)
        part = (wide % 8) // 2
        for p in range(slots):
            chosen = jnp.where(before == float(p), member, 0.0)
            weight = jnp.sum(chosen * gates, axis=1, keepdims=True)
            scale_ref[p] = jnp.where(is_cot[:, :1], weight, 1.0)
            kept = jnp.concatenate([jnp.where(is_cot, 0.0, chosen), jnp.where(is_cot, chosen, 0.0)], axis=1)
            for q in range(4):
                pick_ref[p, :, q * 2 * n_tok : (q + 1) * 2 * n_tok] = jnp.where(part == q, kept, 0.0).astype(BF)

    source = jnp.concatenate([s[...] for s in sources], axis=0)
    p = 0
    for out, count in zip(outs, split):
        for k in range(count):
            picked = nn(pick_ref[p], source) * scale_ref[p]
            out[:, :, k * lanes : (k + 1) * lanes] = picked.reshape(experts, 8, lanes).astype(BF)
            p += 1


def dispatch(ids2, gates2, tokens, cotangent, experts, split):
    n_tok, d = tokens.shape
    lanes = d // 4 // STEPS
    rows = experts * 8
    slots = sum(split)
    columns = []
    for q in range(4):
        columns += [pl.BlockSpec((n_tok, lanes), lambda i, q=q: (0, q * STEPS + i))] * 2
    return pl.pallas_call(
        functools.partial(dispatch_kernel, split),
        grid=(STEPS,),
        in_specs=[pl.BlockSpec((2, n_tok), lambda i: (0, 0))] * 2 + columns,
        out_specs=[pl.BlockSpec((experts, 8, c * lanes), lambda i: (0, 0, i)) for c in split],
        out_shape=[jax.ShapeDtypeStruct((experts, 8, c * d // 4), BF) for c in split],
        scratch_shapes=[pltpu.VMEM((slots, rows, 8 * n_tok), BF), pltpu.VMEM((slots, rows, 1), F32)],
        cost_estimate=cost(2 * slots * rows * 8 * n_tok * d // 4, 4 * n_tok * d * 2 + 2 * slots * experts * d * 2),
        name="dispatch",
    )(ids2, gates2, *([tokens, cotangent] * 4))


def stack_kernel(at_ref, *refs):
    wg, wu, wd, (out, whole) = refs[:PARTS], refs[PARTS : 2 * PARTS], refs[2 * PARTS : 3 * PARTS], refs[-2:]
    width, ff = wg[0].shape
    part, d = wd[0].shape
    for k in range(PARTS):
        owner = lax.rem(at_ref[0] - k + PARTS, PARTS)
        rows = pl.ds(pl.multiple_of(owner * width, width), width)
        out[rows, 0:ff] = wg[k][...]
        out[rows, ff:] = wu[k][...]
        whole[pl.ds(pl.multiple_of(owner * part, part), part), :] = wd[k][...]
    for b in range(d // (2 * ff)):
        for h in range(2):
            col = (2 * b + h) * ff
            out[d + b * ff : d + (b + 1) * ff, h * ff : (h + 1) * ff] = whole[:, col : col + ff].T


def stack(t, wg, wu, wd):
    _, ff = wg[0].shape
    d = wd[0].shape[1]
    return pl.pallas_call(
        stack_kernel,
        in_specs=[SMEM] + [VMEM] * (3 * PARTS),
        out_specs=VMEM,
        out_shape=struct(d + d // 2, 2 * ff),
        scratch_shapes=[pltpu.VMEM((ff, d), BF)],
        cost_estimate=cost(3 * d * ff, 12 * d * ff),
        name="stack",
    )(t, *wg, *wu, *wd)


def widen(recv_ref, flat):
    for b in range(flat.shape[0]):
        flat[b] = recv_ref[:, :, b * 128 : (b + 1) * 128].astype(F32).reshape(flat.shape[1:])


def unpack(flat, sources, q, kinds):
    d = kinds[0][1].shape[1]
    count = kinds[0][1].shape[0] // sources
    lanes = d // 4 // STEPS
    blocks = lanes // 128
    for step in range(STEPS):
        for p in range(count):
            for b in range(blocks):
                col = q * (d // 4) + step * lanes + b * 128
                for kind, dst in kinds:
                    v = flat[(step * count + p) * blocks + b, pl.ds(2 * q + kind, sources, stride=8), :]
                    dst[p * sources : (p + 1) * sources, col : col + 128] = v.astype(BF)


def flat_scratch(recv):
    return pltpu.VMEM((recv.shape[2] // 128, recv.shape[0] * 8, 128), F32)


def expert_kernel(count, recv_ref, w_ref, msg_ref, h_ref, flat, x, c, back, ret, wgu, wd, sem_w):
    sources = recv_ref.shape[0]
    d = x.shape[1]
    width = d // 4
    ff = wgu.shape[1] // 2
    weights_in = [
        pltpu.make_async_copy(
            w_ref.at[pl.ds(q * width, width), :], wgu.at[pl.ds(q * width, width), :], sem_w.at[q]
        )
        for q in range(4)
    ] + [pltpu.make_async_copy(w_ref.at[pl.ds(d, d // 2), :], wd, sem_w.at[4])]
    for copy in weights_in[::-1]:
        copy.start()
    widen(recv_ref, flat)
    for q in range(4):
        unpack(flat, sources, q, [(1, c), (0, x)])
    weights_in[4].wait()
    grad_hidden = jnp.zeros((x.shape[0], ff), F32)
    for b in range(d // (2 * ff)):
        for h in range(2):
            col = (2 * b + h) * ff
            grad_hidden += nn(c[:, col : col + ff], wd[b * ff : (b + 1) * ff, h * ff : (h + 1) * ff])
    pre = jnp.zeros((x.shape[0], 2 * ff), F32)
    for q in range(4)[::-1]:
        weights_in[q].wait()
        cols = slice(q * width, (q + 1) * width)
        pre += nn(x[:, cols], wgu[cols, :])
    pre_gate, pre_up = pre[:, :ff], pre[:, ff:]
    sig = jax.nn.sigmoid(pre_gate)
    activated = pre_gate * sig
    grad_gate_pre = (grad_hidden * pre_up * sig * (1.0 + pre_gate * (1.0 - sig))).astype(BF)
    grad_up_pre = (grad_hidden * activated).astype(BF)
    hidden = (activated * pre_up).astype(BF)
    both = jnp.concatenate([grad_gate_pre, grad_up_pre], axis=1)
    for q in range(4):
        cols = slice(q * width, (q + 1) * width)
        back[:, cols] = nt(both, wgu[cols, :])
    eighth = d // 8
    blocks = eighth // 128
    for p in range(count):
        for b in range(blocks):
            for o in range(8):
                col = o * eighth + b * 128
                ret[p * blocks + b, pl.ds(o, sources, stride=8), :] = back[p * sources : (p + 1) * sources, col : col + 128]
        for b in range(blocks):
            at = p * eighth + b * 128
            msg_ref[:, :, at : at + 128] = ret[p * blocks + b].reshape(sources, 8, 128).astype(BF)
    h_ref[:, 0:ff] = hidden
    h_ref[:, ff:] = both


def expert_round(recv, weights, ff, count):
    sources = recv.shape[0]
    d = recv.shape[2] * 4 // count
    rows = sources * count
    return pl.pallas_call(
        functools.partial(expert_kernel, count),
        in_specs=[VMEM, HBM],
        out_specs=[VMEM] * 2,
        out_shape=[struct(sources, 8, count * d // 8), struct(rows, 3 * ff)],
        scratch_shapes=[
            flat_scratch(recv),
            pltpu.VMEM((rows, d), BF),
            pltpu.VMEM((rows, d), BF),
            pltpu.VMEM((rows, d), F32),
            pltpu.VMEM((count * d // 8 // 128, sources * 8, 128), F32),
            pltpu.VMEM((d, 2 * ff), BF),
            pltpu.VMEM((d // 2, 2 * ff), BF),
            pltpu.SemaphoreType.DMA((5,)),
        ],
        cost_estimate=cost(2 * rows * d * 5 * ff, 3 * ff * d * 2 + 3 * rows * d * 2),
        compiler_params=pltpu.CompilerParams(vmem_limit_bytes=50 << 20),
        name="expert_round",
    )(recv, weights)


def spread_kernel(kind, first, wide, t_ref, recv_ref, h_ref, *refs):
    boxes, (flat, x) = refs[:PARTS], refs[PARTS:]
    widen(recv_ref, flat)
    for q in range(4):
        unpack(flat, recv_ref.shape[0], q, [(kind, x)])
    rows, d = x.shape
    width = d // PARTS
    folds = width // wide
    part = rows // folds
    for k in range(PARTS):
        there = pl.ds(pl.multiple_of(lax.rem(t_ref[0] + k, PARTS) * width, width), width)
        boxes[k][0:rows, :] = x[:, there]
        for f in range(folds):
            boxes[k][rows:, f * wide : (f + 1) * wide] = h_ref[f * part : (f + 1) * part, first : first + wide]


def spread(t, recv, h, kind, first, wide):
    rows = h.shape[0]
    d = recv.shape[2] * 8 * recv.shape[0] // (2 * rows)
    width = d // PARTS
    return list(
        pl.pallas_call(
            functools.partial(spread_kernel, kind, first, wide),
            in_specs=[SMEM] + [VMEM] * 2,
            out_specs=[VMEM] * PARTS,
            out_shape=[struct(rows + rows * wide // width, width)] * PARTS,
            scratch_shapes=[flat_scratch(recv), pltpu.VMEM((rows, d), BF)],
            cost_estimate=cost(rows * d, 6 * rows * d),
            compiler_params=pltpu.CompilerParams(vmem_limit_bytes=50 << 20),
        )(t, recv, h)
    )


def join(boxes, x, h):
    rows = x.shape[0] // len(boxes)
    wide = h.shape[1]
    folds = x.shape[1] // wide
    part = rows // folds
    for i, box in enumerate(boxes):
        x[i * rows : (i + 1) * rows, :] = box[0:rows, :]
        for f in range(folds):
            h[i * rows + f * part : i * rows + (f + 1) * part, :] = box[rows:, f * wide : (f + 1) * wide]


def grads_down_kernel(t_ref, *refs):
    boxes, downs, (c, h) = refs[:PARTS], refs[PARTS : 2 * PARTS], refs[2 * PARTS :]
    join(boxes, c, h)
    ff = h.shape[1]
    c[0:ff, :] = tn(h[...], c[...]).astype(BF)
    part = ff // PARTS
    for k in range(PARTS):
        downs[k][...] = c[pl.ds(pl.multiple_of(lax.rem(t_ref[0] + k, PARTS) * part, part), part), :]


def grads_up_kernel(*refs):
    boxes, (gg_ref, gu_ref, x, h) = refs[:PARTS], refs[PARTS:]
    join(boxes, x, h)
    ff = gg_ref.shape[1]
    gg_ref[...] = tn(x[...], h[:, :ff]).astype(BF)
    gu_ref[...] = tn(x[...], h[:, ff:]).astype(BF)


def grads_down(t, boxes, rows, ff):
    width = boxes[0].shape[1]
    rows *= PARTS
    return pl.pallas_call(
        grads_down_kernel,
        in_specs=[SMEM] + [VMEM] * PARTS,
        out_specs=[VMEM] * PARTS,
        out_shape=[struct(ff // PARTS, width)] * PARTS,
        scratch_shapes=[pltpu.VMEM((rows, width), BF), pltpu.VMEM((rows, ff), BF)],
        cost_estimate=cost(2 * rows * width * ff, 2 * rows * width * 2),
        name="grads_down",
    )(t, *boxes)


def grads_up(boxes, rows, ff):
    width = boxes[0].shape[1]
    rows *= PARTS
    return pl.pallas_call(
        grads_up_kernel,
        in_specs=[VMEM] * PARTS,
        out_specs=[VMEM] * 2,
        out_shape=[struct(width, ff)] * 2,
        scratch_shapes=[pltpu.VMEM((rows, width), BF), pltpu.VMEM((rows, 2 * ff), BF)],
        cost_estimate=cost(4 * rows * width * ff, 3 * rows * width * 2),
        name="grads_up",
    )(*boxes)


def pick_kernel(experts, ids_ref, pick_ref):
    n_tok, rows = pick_ref.shape
    lane = lax.broadcasted_iota(jnp.int32, (n_tok, rows), 1)
    expert = lane % experts
    member = jnp.where((ids_ref[:, 0:1] == expert) | (ids_ref[:, 1:2] == expert), 1.0, 0.0).astype(F32)
    i = lax.broadcasted_iota(jnp.int32, (n_tok, n_tok), 0)
    j = lax.broadcasted_iota(jnp.int32, (n_tok, n_tok), 1)
    before = nn(jnp.where(j < i, 1.0, 0.0).astype(BF), member.astype(BF))
    pick_ref[...] = jnp.where(before == (lane // experts).astype(F32), member, 0.0).astype(BF)


def pick(ids, experts, slots):
    n_tok = ids.shape[0]
    return pl.pallas_call(
        functools.partial(pick_kernel, experts),
        in_specs=[VMEM],
        out_specs=VMEM,
        out_shape=struct(n_tok, slots * experts),
        cost_estimate=cost(2 * n_tok * n_tok * slots * experts, 4 * n_tok * slots * experts),
        name="pick",
    )(ids)


def combine_kernel(pick_ref, ret_ref, out_ref, flat, rhs):
    experts = ret_ref.shape[0]
    eighth = out_ref.shape[1] // 8
    blocks = eighth // 128
    for b in range(flat.shape[0]):
        flat[b] = ret_ref[:, :, b * 128 : (b + 1) * 128].astype(F32).reshape(flat.shape[1:])
    for o in range(8):
        for b in range(blocks):
            col = o * eighth + b * 128
            for p in range(flat.shape[0] // blocks):
                v = flat[p * blocks + b, pl.ds(o, experts, stride=8), :]
                rhs[p * experts : (p + 1) * experts, col : col + 128] = v.astype(BF)
    out_ref[...] = nn(pick_ref[...], rhs[...]).astype(BF)


def combine(picks, ret, d):
    n_tok, rows = picks.shape
    return pl.pallas_call(
        combine_kernel,
        in_specs=[VMEM] * 2,
        out_specs=VMEM,
        out_shape=struct(n_tok, d),
        scratch_shapes=[pltpu.VMEM((ret.shape[2] // 128, ret.shape[0] * 8, 128), F32), pltpu.VMEM((rows, d), BF)],
        cost_estimate=cost(2 * n_tok * rows * d, 4 * n_tok * d * 2),
        compiler_params=pltpu.CompilerParams(vmem_limit_bytes=14 << 20),
        name="combine",
    )(picks, ret)


def place_kernel(t_ref, *refs):
    out = refs[-1]
    width = refs[0].shape[1]
    for k in range(PARTS):
        at = pl.multiple_of(lax.rem(t_ref[0] - k + PARTS, PARTS) * width, width)
        out[:, pl.ds(at, width)] = refs[k][...]


def place(t, pieces):
    rows, width = pieces[0].shape
    return pl.pallas_call(
        place_kernel,
        in_specs=[SMEM] + [VMEM] * len(pieces),
        out_specs=VMEM,
        out_shape=jax.ShapeDtypeStruct((rows, width * len(pieces)), BF),
        cost_estimate=cost(rows * width, 4 * rows * width * 4),
        name="place",
    )(t, *pieces)


def local(tokens, cotangent, expert_ids, gate_wts, w_gate, w_up, w_down):
    n_tok, d = tokens.shape
    experts = lax.axis_size("expert")
    slots = 2 * n_tok // experts
    split = (slots,)
    t = lax.axis_index("tensor").astype(jnp.int32).reshape(1)
    ff = w_gate.shape[2]

    def shift(x, k):
        return lax.ppermute(x, "tensor", [(s, (s + k) % PARTS) for s in range(PARTS)])

    def everyone(x):
        return [x] + [shift(x, k) for k in range(1, PARTS)]

    sends = dispatch(expert_ids.T, gate_wts.T, tokens, cotangent, experts, split)
    recvs = []
    for send in sends:
        recvs.append(lax.all_to_all(send, "expert", 0, 0, tiled=True))
    wg, wu, wd = everyone(w_gate[0]), everyone(w_up[0]), everyone(w_down[0])
    weights = stack(t, wg, wu, wd)
    (recv,), (count,) = recvs, split
    msg, h = expert_round(recv, weights, ff, count)
    ret = lax.all_to_all(msg, "expert", 0, 0, tiled=True)
    picks = pick(expert_ids, experts, slots)
    boxes_c = spread(t, recv, h, 1, 0, ff)
    boxes_c = boxes_c[:1] + [shift(boxes_c[k], k) for k in range(1, PARTS)]
    boxes_x = spread(t, recv, h, 0, ff, 2 * ff)
    boxes_x = boxes_x[:1] + [shift(boxes_x[k], k) for k in range(1, PARTS)]
    down = grads_down(t, boxes_c, h.shape[0], ff)
    down = list(down[:1]) + [shift(down[k], k) for k in range(1, PARTS)]
    grad_gate, grad_up = grads_up(boxes_x, h.shape[0], ff)
    grad_down = place(t, down)
    input_grad = combine(picks, ret, d)
    return input_grad, grad_gate[None], grad_up[None], grad_down[None]


def solution(mesh):
    tok = P(("group", "expert", "tensor"), None)
    wts = P("expert", "tensor", None)
    out = P(("group", "expert"), "tensor", None)

    return jax.shard_map(
        local,
        mesh=mesh,
        in_specs=(tok, tok, tok, tok, wts, wts, wts),
        out_specs=(tok, out, out, out),
        check_vma=False,
    )
```

```python
import functools

import jax
import jax.numpy as jnp
from jax import lax
from jax.experimental import pallas as pl
from jax.experimental.pallas import tpu as pltpu
from jax.sharding import PartitionSpec as P


BF = jnp.bfloat16
F32 = jnp.float32
VMEM = pl.BlockSpec(memory_space=pltpu.VMEM)
SMEM = pl.BlockSpec(memory_space=pltpu.SMEM)
HBM = pl.BlockSpec(memory_space=pltpu.HBM)
PARTS = 4
STEPS = 2


def cost(flops, bytes_accessed):
    return pl.CostEstimate(flops=int(flops), bytes_accessed=int(bytes_accessed), transcendentals=0)


def struct(*shape):
    return jax.ShapeDtypeStruct(shape, BF)


def nn(a, b):
    return lax.dot_general(a, b, (((1,), (0,)), ((), ())), preferred_element_type=F32)


def nt(a, b):
    return lax.dot_general(a, b, (((1,), (1,)), ((), ())), preferred_element_type=F32)


def tn(a, b):
    return lax.dot_general(a, b, (((0,), (0,)), ((), ())), preferred_element_type=F32)


def dispatch_kernel(split, ids_ref, gate_ref, *refs):
    sources, refs = refs[:8], refs[8:]
    outs, (pick_ref, scale_ref) = refs[: len(split)], refs[len(split) + 1 :]
    n_tok, lanes = sources[0].shape
    experts = outs[0].shape[0]
    rows = experts * 8
    slots = sum(split)

    @pl.when(pl.program_id(0) == 0)
    def _():
        row = lax.broadcasted_iota(jnp.int32, (rows, n_tok), 0)
        expert = row // 8
        first = ids_ref[0:1, :] == expert
        second = ids_ref[1:2, :] == expert
        member = jnp.where(first | second, 1.0, 0.0).astype(F32)
        j = lax.broadcasted_iota(jnp.int32, (n_tok, n_tok), 0)
        i = lax.broadcasted_iota(jnp.int32, (n_tok, n_tok), 1)
        before = nn(member.astype(BF), jnp.where(j < i, 1.0, 0.0).astype(BF))
        gates = jnp.where(first, gate_ref[0:1, :], gate_ref[1:2, :])
        is_cot = row % 2 == 1
        wide = lax.broadcasted_iota(jnp.int32, (rows, 2 * n_tok), 0)
        part = (wide % 8) // 2
        for p in range(slots):
            chosen = jnp.where(before == float(p), member, 0.0)
            weight = jnp.sum(chosen * gates, axis=1, keepdims=True)
            scale_ref[p] = jnp.where(is_cot[:, :1], weight, 1.0)
            kept = jnp.concatenate([jnp.where(is_cot, 0.0, chosen), jnp.where(is_cot, chosen, 0.0)], axis=1)
            for q in range(4):
                pick_ref[p, :, q * 2 * n_tok : (q + 1) * 2 * n_tok] = jnp.where(part == q, kept, 0.0).astype(BF)

    source = jnp.concatenate([s[...] for s in sources], axis=0)
    p = 0
    for out, count in zip(outs, split):
        for k in range(count):
            picked = nn(pick_ref[p], source) * scale_ref[p]
            out[:, :, k * lanes : (k + 1) * lanes] = picked.reshape(experts, 8, lanes).astype(BF)
            p += 1


def dispatch(ids2, gates2, tokens, cotangent, experts, split):
    n_tok, d = tokens.shape
    lanes = d // 4 // STEPS
    rows = experts * 8
    slots = sum(split)
    columns = []
    for q in range(4):
        columns += [pl.BlockSpec((n_tok, lanes), lambda i, q=q: (0, q * STEPS + i))] * 2
    return pl.pallas_call(
        functools.partial(dispatch_kernel, split),
        grid=(STEPS,),
        in_specs=[pl.BlockSpec((2, n_tok), lambda i: (0, 0))] * 2 + columns,
        out_specs=[pl.BlockSpec((experts, 8, c * lanes), lambda i: (0, 0, i)) for c in split] + [HBM],
        out_shape=[struct(experts, 8, c * d // 4) for c in split] + [struct(experts, 8, slots * d // 8)],
        scratch_shapes=[pltpu.VMEM((slots, rows, 8 * n_tok), BF), pltpu.VMEM((slots, rows, 1), F32)],
        cost_estimate=cost(2 * slots * rows * 8 * n_tok * d // 4, 4 * n_tok * d * 2 + 2 * slots * experts * d * 2),
        name="dispatch",
    )(ids2, gates2, *([tokens, cotangent] * 4))


def stack_kernel(at_ref, *refs):
    wg, wu, wd, (out, whole) = refs[:PARTS], refs[PARTS : 2 * PARTS], refs[2 * PARTS : 3 * PARTS], refs[-2:]
    width, ff = wg[0].shape
    part, d = wd[0].shape
    for k in range(PARTS):
        owner = lax.rem(at_ref[0] - k + PARTS, PARTS)
        rows = pl.ds(pl.multiple_of(owner * width, width), width)
        out[rows, 0:ff] = wg[k][...]
        out[rows, ff:] = wu[k][...]
        whole[pl.ds(pl.multiple_of(owner * part, part), part), :] = wd[k][...]
    for b in range(d // (2 * ff)):
        for h in range(2):
            col = (2 * b + h) * ff
            out[d + b * ff : d + (b + 1) * ff, h * ff : (h + 1) * ff] = whole[:, col : col + ff].T


def stack(t, wg, wu, wd):
    _, ff = wg[0].shape
    d = wd[0].shape[1]
    return pl.pallas_call(
        stack_kernel,
        in_specs=[SMEM] + [VMEM] * (3 * PARTS),
        out_specs=VMEM,
        out_shape=struct(d + d // 2, 2 * ff),
        scratch_shapes=[pltpu.VMEM((ff, d), BF)],
        cost_estimate=cost(3 * d * ff, 12 * d * ff),
        name="stack",
    )(t, *wg, *wu, *wd)


def widen(recv_ref, flat):
    for b in range(flat.shape[0]):
        flat[b] = recv_ref[:, :, b * 128 : (b + 1) * 128].astype(F32).reshape(flat.shape[1:])


def unpack(flat, sources, q, kinds):
    d = kinds[0][1].shape[1]
    count = kinds[0][1].shape[0] // sources
    lanes = d // 4 // STEPS
    blocks = lanes // 128
    for step in range(STEPS):
        for p in range(count):
            for b in range(blocks):
                col = q * (d // 4) + step * lanes + b * 128
                for kind, dst in kinds:
                    v = flat[(step * count + p) * blocks + b, pl.ds(2 * q + kind, sources, stride=8), :]
                    dst[p * sources : (p + 1) * sources, col : col + 128] = v.astype(BF)


def flat_scratch(recv):
    return pltpu.VMEM((recv.shape[2] // 128, recv.shape[0] * 8, 128), F32)


def expert_kernel(count, recv_ref, w_ref, spare_ref, msg_ref, h_ref, flat, x, c, ret, msg, wgu, wd, sem_w, sem_out):
    sources = recv_ref.shape[0]
    d = x.shape[1]
    width = d // 4
    ff = wgu.shape[1] // 2
    weights_in = [
        pltpu.make_async_copy(
            w_ref.at[pl.ds(q * width, width), :], wgu.at[pl.ds(q * width, width), :], sem_w.at[q]
        )
        for q in range(4)
    ] + [pltpu.make_async_copy(w_ref.at[pl.ds(d, d // 2), :], wd, sem_w.at[4])]
    for copy in weights_in[::-1]:
        copy.start()
    widen(recv_ref, flat)
    for q in range(4):
        unpack(flat, sources, q, [(1, c), (0, x)])
    weights_in[4].wait()
    grad_hidden = jnp.zeros((x.shape[0], ff), F32)
    for b in range(d // (2 * ff)):
        for h in range(2):
            col = (2 * b + h) * ff
            grad_hidden += nn(c[:, col : col + ff], wd[b * ff : (b + 1) * ff, h * ff : (h + 1) * ff])
    pre = jnp.zeros((x.shape[0], 2 * ff), F32)
    for q in range(4)[::-1]:
        weights_in[q].wait()
        cols = slice(q * width, (q + 1) * width)
        pre += nn(x[:, cols], wgu[cols, :])
    pre_gate, pre_up = pre[:, :ff], pre[:, ff:]
    sig = jax.nn.sigmoid(pre_gate)
    activated = pre_gate * sig
    grad_gate_pre = (grad_hidden * pre_up * sig * (1.0 + pre_gate * (1.0 - sig))).astype(BF)
    grad_up_pre = (grad_hidden * activated).astype(BF)
    hidden = (activated * pre_up).astype(BF)
    both = jnp.concatenate([grad_gate_pre, grad_up_pre], axis=1)
    eighth = d // 8
    blocks = eighth // 128
    for q in range(4):
        rows = nt(both, wgu[q * width : (q + 1) * width, :])
        for p in range(count):
            for b in range(blocks):
                for o in range(2):
                    col = o * eighth + b * 128
                    ret[p * blocks + b, pl.ds(2 * q + o, sources, stride=8), :] = rows[
                        p * sources : (p + 1) * sources, col : col + 128
                    ]
    out = [
        pltpu.make_async_copy(msg.at[p], msg_ref.at[:, :, pl.ds(p * eighth, eighth)], sem_out.at[p]) for p in range(count)
    ]
    for p in range(count):
        for b in range(blocks):
            msg[p, :, :, b * 128 : (b + 1) * 128] = ret[p * blocks + b].reshape(sources, 8, 128).astype(BF)
        if p:
            out[p - 1].start()
    h_ref[:, 0:ff] = hidden
    h_ref[:, ff:] = both
    out[-1].start()
    for copy in out:
        copy.wait()


def expert_round(recv, weights, spare, ff, count):
    sources = recv.shape[0]
    d = recv.shape[2] * 4 // count
    rows = sources * count
    return pl.pallas_call(
        functools.partial(expert_kernel, count),
        in_specs=[VMEM, HBM, HBM],
        out_specs=[HBM, VMEM],
        input_output_aliases={2: 0},
        out_shape=[struct(sources, 8, count * d // 8), struct(rows, 3 * ff)],
        scratch_shapes=[
            flat_scratch(recv),
            pltpu.VMEM((rows, d), BF),
            pltpu.VMEM((rows, d), BF),
            pltpu.VMEM((count * d // 8 // 128, sources * 8, 128), F32),
            pltpu.VMEM((count, sources, 8, d // 8), BF),
            pltpu.VMEM((d, 2 * ff), BF),
            pltpu.VMEM((d // 2, 2 * ff), BF),
            pltpu.SemaphoreType.DMA((5,)),
            pltpu.SemaphoreType.DMA((count,)),
        ],
        cost_estimate=cost(2 * rows * d * 5 * ff, 3 * ff * d * 2 + 3 * rows * d * 2),
        compiler_params=pltpu.CompilerParams(vmem_limit_bytes=50 << 20),
        name="expert_round",
    )(recv, weights, spare)


def spread_kernel(kind, first, wide, t_ref, recv_ref, h_ref, *refs):
    boxes, (flat, x) = refs[:PARTS], refs[PARTS:]
    widen(recv_ref, flat)
    for q in range(4):
        unpack(flat, recv_ref.shape[0], q, [(kind, x)])
    rows, d = x.shape
    width = d // PARTS
    folds = width // wide
    part = rows // folds
    for k in range(PARTS):
        there = pl.ds(pl.multiple_of(lax.rem(t_ref[0] + k, PARTS) * width, width), width)
        boxes[k][0:rows, :] = x[:, there]
        for f in range(folds):
            boxes[k][rows:, f * wide : (f + 1) * wide] = h_ref[f * part : (f + 1) * part, first : first + wide]


def spread(t, recv, h, kind, first, wide):
    rows = h.shape[0]
    d = recv.shape[2] * 8 * recv.shape[0] // (2 * rows)
    width = d // PARTS
    return list(
        pl.pallas_call(
            functools.partial(spread_kernel, kind, first, wide),
            in_specs=[SMEM] + [VMEM] * 2,
            out_specs=[VMEM] * PARTS,
            out_shape=[struct(rows + rows * wide // width, width)] * PARTS,
            scratch_shapes=[flat_scratch(recv), pltpu.VMEM((rows, d), BF)],
            cost_estimate=cost(rows * d, 6 * rows * d),
            compiler_params=pltpu.CompilerParams(vmem_limit_bytes=50 << 20),
        )(t, recv, h)
    )


def join(boxes, x, h):
    rows = x.shape[0] // len(boxes)
    wide = h.shape[1]
    folds = x.shape[1] // wide
    part = rows // folds
    for i, box in enumerate(boxes):
        x[i * rows : (i + 1) * rows, :] = box[0:rows, :]
        for f in range(folds):
            h[i * rows + f * part : i * rows + (f + 1) * part, :] = box[rows:, f * wide : (f + 1) * wide]


def grads_down_kernel(t_ref, *refs):
    boxes, downs, (c, h) = refs[:PARTS], refs[PARTS : 2 * PARTS], refs[2 * PARTS :]
    join(boxes, c, h)
    ff = h.shape[1]
    c[0:ff, :] = tn(h[...], c[...]).astype(BF)
    part = ff // PARTS
    for k in range(PARTS):
        downs[k][...] = c[pl.ds(pl.multiple_of(lax.rem(t_ref[0] + k, PARTS) * part, part), part), :]


def grads_up_kernel(*refs):
    boxes, (gg_ref, gu_ref, x, h) = refs[:PARTS], refs[PARTS:]
    join(boxes, x, h)
    ff = gg_ref.shape[1]
    gg_ref[...] = tn(x[...], h[:, :ff]).astype(BF)
    gu_ref[...] = tn(x[...], h[:, ff:]).astype(BF)


def grads_down(t, boxes, rows, ff):
    width = boxes[0].shape[1]
    rows *= PARTS
    return pl.pallas_call(
        grads_down_kernel,
        in_specs=[SMEM] + [VMEM] * PARTS,
        out_specs=[VMEM] * PARTS,
        out_shape=[struct(ff // PARTS, width)] * PARTS,
        scratch_shapes=[pltpu.VMEM((rows, width), BF), pltpu.VMEM((rows, ff), BF)],
        cost_estimate=cost(2 * rows * width * ff, 2 * rows * width * 2),
        name="grads_down",
    )(t, *boxes)


def grads_up(boxes, rows, ff):
    width = boxes[0].shape[1]
    rows *= PARTS
    return pl.pallas_call(
        grads_up_kernel,
        in_specs=[VMEM] * PARTS,
        out_specs=[VMEM] * 2,
        out_shape=[struct(width, ff)] * 2,
        scratch_shapes=[pltpu.VMEM((rows, width), BF), pltpu.VMEM((rows, 2 * ff), BF)],
        cost_estimate=cost(4 * rows * width * ff, 3 * rows * width * 2),
        name="grads_up",
    )(*boxes)


def pick_kernel(experts, ids_ref, pick_ref):
    n_tok, rows = pick_ref.shape
    lane = lax.broadcasted_iota(jnp.int32, (n_tok, rows), 1)
    expert = lane % experts
    member = jnp.where((ids_ref[:, 0:1] == expert) | (ids_ref[:, 1:2] == expert), 1.0, 0.0).astype(F32)
    i = lax.broadcasted_iota(jnp.int32, (n_tok, n_tok), 0)
    j = lax.broadcasted_iota(jnp.int32, (n_tok, n_tok), 1)
    before = nn(jnp.where(j < i, 1.0, 0.0).astype(BF), member.astype(BF))
    pick_ref[...] = jnp.where(before == (lane // experts).astype(F32), member, 0.0).astype(BF)


def pick(ids, experts, slots):
    n_tok = ids.shape[0]
    return pl.pallas_call(
        functools.partial(pick_kernel, experts),
        in_specs=[VMEM],
        out_specs=VMEM,
        out_shape=struct(n_tok, slots * experts),
        cost_estimate=cost(2 * n_tok * n_tok * slots * experts, 4 * n_tok * slots * experts),
        name="pick",
    )(ids)


def combine_kernel(pick_ref, ret_ref, out_ref, flat, rhs):
    experts = ret_ref.shape[0]
    eighth = out_ref.shape[1] // 8
    blocks = eighth // 128
    for b in range(flat.shape[0]):
        flat[b] = ret_ref[:, :, b * 128 : (b + 1) * 128].astype(F32).reshape(flat.shape[1:])
    for o in range(8):
        for b in range(blocks):
            col = o * eighth + b * 128
            for p in range(flat.shape[0] // blocks):
                v = flat[p * blocks + b, pl.ds(o, experts, stride=8), :]
                rhs[p * experts : (p + 1) * experts, col : col + 128] = v.astype(BF)
    out_ref[...] = nn(pick_ref[...], rhs[...]).astype(BF)


def combine(picks, ret, d):
    n_tok, rows = picks.shape
    return pl.pallas_call(
        combine_kernel,
        in_specs=[VMEM] * 2,
        out_specs=VMEM,
        out_shape=struct(n_tok, d),
        scratch_shapes=[pltpu.VMEM((ret.shape[2] // 128, ret.shape[0] * 8, 128), F32), pltpu.VMEM((rows, d), BF)],
        cost_estimate=cost(2 * n_tok * rows * d, 4 * n_tok * d * 2),
        compiler_params=pltpu.CompilerParams(vmem_limit_bytes=14 << 20),
        name="combine",
    )(picks, ret)


def place_kernel(t_ref, *refs):
    out = refs[-1]
    width = refs[0].shape[1]
    for k in range(PARTS):
        at = pl.multiple_of(lax.rem(t_ref[0] - k + PARTS, PARTS) * width, width)
        out[:, pl.ds(at, width)] = refs[k][...]


def place(t, pieces):
    rows, width = pieces[0].shape
    return pl.pallas_call(
        place_kernel,
        in_specs=[SMEM] + [VMEM] * len(pieces),
        out_specs=VMEM,
        out_shape=jax.ShapeDtypeStruct((rows, width * len(pieces)), BF),
        cost_estimate=cost(rows * width, 4 * rows * width * 4),
        name="place",
    )(t, *pieces)


def local(tokens, cotangent, expert_ids, gate_wts, w_gate, w_up, w_down):
    n_tok, d = tokens.shape
    experts = lax.axis_size("expert")
    slots = 2 * n_tok // experts
    split = (slots,)
    t = lax.axis_index("tensor").astype(jnp.int32).reshape(1)
    ff = w_gate.shape[2]

    def shift(x, k):
        return lax.ppermute(x, "tensor", [(s, (s + k) % PARTS) for s in range(PARTS)])

    def everyone(x):
        return [x] + [shift(x, k) for k in range(1, PARTS)]

    *sends, spare = dispatch(expert_ids.T, gate_wts.T, tokens, cotangent, experts, split)
    recvs = []
    for send in sends:
        recvs.append(lax.all_to_all(send, "expert", 0, 0, tiled=True))
    wg, wu, wd = everyone(w_gate[0]), everyone(w_up[0]), everyone(w_down[0])
    weights = stack(t, wg, wu, wd)
    (recv,), (count,) = recvs, split
    msg, h = expert_round(recv, weights, spare, ff, count)
    ret = lax.all_to_all(msg, "expert", 0, 0, tiled=True)
    picks = pick(expert_ids, experts, slots)
    boxes_c = spread(t, recv, h, 1, 0, ff)
    boxes_c = boxes_c[:1] + [shift(boxes_c[k], k) for k in range(1, PARTS)]
    boxes_x = spread(t, recv, h, 0, ff, 2 * ff)
    boxes_x = boxes_x[:1] + [shift(boxes_x[k], k) for k in range(1, PARTS)]
    down = grads_down(t, boxes_c, h.shape[0], ff)
    down = list(down[:1]) + [shift(down[k], k) for k in range(1, PARTS)]
    grad_gate, grad_up = grads_up(boxes_x, h.shape[0], ff)
    grad_down = place(t, down)
    input_grad = combine(picks, ret, d)
    return input_grad, grad_gate[None], grad_up[None], grad_down[None]


def solution(mesh):
    tok = P(("group", "expert", "tensor"), None)
    wts = P("expert", "tensor", None)
    out = P(("group", "expert"), "tensor", None)

    return jax.shard_map(
        local,
        mesh=mesh,
        in_specs=(tok, tok, tok, tok, wts, wts, wts),
        out_specs=(tok, out, out, out),
        check_vma=False,
    )
```
